32 devices in a mesh: groups: 2 (over y), dp: 8 (over z, core), expert: 2 (over x).
Axes of the slice: x: 2, y: 2, z: 4, core: 2. Of those that a mesh axis runs over, the one named last changes fastest.
Arguments:
- queries: bfloat16 [2, 256, 32, 128], P(None, ('groups', 'dp'), 'expert'), parts along dimension 1, may hold values from -6 to 6
- fresh_kv: bfloat16 [2, 256, 4, 256], P(None, ('groups', 'dp'), 'expert'), parts along dimension 1, may hold values from -6 to 6
- kv_pool: bfloat16 [5120, 16, 4, 256], P(('groups', 'dp'), None, 'expert'), parts along dimension 0, may hold values from -6 to 6
- page_table: int32 [256, 305], P(('groups', 'dp')), parts along dimension 0, may hold values from -1 to 319, as said below
- context_lengths: int32 [256], P(('groups', 'dp')), parts along dimension 0, may hold values from 1 to 4880, as said below
- residual: bfloat16 [2, 256, 4096], P(None, ('groups', 'dp'), 'expert'), parts along dimension 1, may hold values from -16 to 16
- out_weight: bfloat16 [4096, 4096], P('expert', 'dp'), may hold values from -0.09375 to 0.09375
- norm_gain: float32 [4096], P('expert'), may hold values from 0.1 to 1.9
- expert_ids: int32 [2, 256, 8], P(None, ('groups', 'dp')), parts along dimension 1, may hold values from 0 to 15, all different within a row; in each aligned block of 16 rows (0 to 15, 16 to 31, ..., all dimensions but the last counted through in order) at most 16 rows name the same one
- route_weights: float32 [2, 256, 8], P(None, ('groups', 'dp')), parts along dimension 1, may hold values from 0.1 to 1
- gate_up: bfloat16 [16, 2, 4096, 768], P('dp', None, 'expert'), may hold values from -0.09375 to 0.09375
- down_proj: bfloat16 [16, 768, 4096], P('dp', None, 'expert'), may hold values from -0.21875 to 0.21875
Outputs:
- layer_out: bfloat16 [2, 256, 4096], P(None, ('groups', 'dp'), 'expert'), parts along dimension 1
The draws below stay inside these ranges and needn't reach their ends.
There are 2 independent parts, one for each index of `groups`. The reference program is written for one: setup_inputs(seed, part) draws one part's arguments, and reference() takes and returns one part's arrays. A program takes and returns all parts, laid end to end along the dimension named above; an argument that names none is the same for every part. Nothing has to cross between parts.
Inputs may be any that keep to these rules, and one draw needn't show every extreme that they name: `page_table`: entries 0 to ceil(context_lengths[i] / 16) - 1 of a row name distinct pages, no page is named twice within the 16 requests of one block, and later entries are -1. The requests of one block hold at most 320 pages together; in every draw some block holds exactly 320, and some request holds exactly 305 pages. `context_lengths`: every request holds at least one cached token; in every draw some request holds exactly 4880. `expert_ids`: within the rows of one device (16 requests of one step) no expert is named by more than 16 rows.
All inputs are finite; a program needn't handle non-finite values.
Results may differ from the reference program's by a relative error of at most 0.005.
Values may be sent and summed in bfloat16 or wider, within the bound.
No kernel may reach another device: no remote copies, remote signals or barrier semaphores. Data moves between devices by JAX's collectives and lax.ppermute only.
A program may use at most 64 MiB of HBM per device.

```python
import math
import jax
import jax.numpy as jnp
import numpy as np
from jax import lax

D = 4096
HQ = 32
KVH = 4
HD = 128
HID = 768
TOP = 8
PAGE = 16
STEPS = 2
REQ_DP = 16
REQS = 128
EXPERTS = 16
POOL = 320
POOL_ALL = 2560
MAXP = 305
CAP = 16
N_DP = 8


def device_layout(device_key, page_total, packed):
    first_key, second_key, third_key = jax.random.split(device_key, 3)
    scores = jax.random.permutation(first_key, POOL).astype(jnp.int32)
    index = jnp.arange(POOL, dtype=jnp.int32)
    allowed = (index >= 1) & (index < page_total)
    ranked = jnp.where(allowed, scores, POOL + index)
    picked = jnp.argsort(ranked, stable=True)[:REQ_DP - 1]
    spread_cuts = jnp.sort(picked).astype(jnp.int32)
    packed_cuts = jnp.arange(1, REQ_DP, dtype=jnp.int32)
    cuts = jnp.where(packed, packed_cuts, spread_cuts).astype(jnp.int32)
    bounds = jnp.concatenate([jnp.zeros((1,), jnp.int32), cuts, jnp.reshape(page_total, (1,)).astype(jnp.int32)])
    counts = bounds[1:] - bounds[:-1]
    order = jax.random.permutation(second_key, POOL).astype(jnp.int32)
    slot_index = jnp.arange(MAXP, dtype=jnp.int32)
    where_in = bounds[:-1, None] + slot_index[None, :]
    live_slot = slot_index[None, :] < counts[:, None]
    table = jnp.where(live_slot, order[jnp.clip(where_in, 0, POOL - 1)], -1).astype(jnp.int32)
    tail = jax.random.randint(third_key, (REQ_DP,), 1, PAGE + 1).astype(jnp.int32)
    last_request = jnp.arange(REQ_DP, dtype=jnp.int32) == REQ_DP - 1
    tail = jnp.where(packed & last_request, PAGE, tail).astype(jnp.int32)
    lengths = ((counts - 1) * PAGE + tail).astype(jnp.int32)
    return (lengths, table)


def pool_layout(key):
    base = jax.random.fold_in(key, 11)
    level_key, busy_key, device_key = jax.random.split(base, 3)
    levels = jax.random.randint(level_key, (N_DP,), 1, 9).astype(jnp.int32)
    busiest = jax.random.randint(busy_key, (), 0, N_DP)
    is_busiest = jnp.arange(N_DP) == busiest
    levels = jnp.where(is_busiest, 8, levels)
    totals = (POOL * levels // 8).astype(jnp.int32)
    device_keys = jax.random.split(device_key, N_DP)
    lengths, table = jax.vmap(device_layout)(device_keys, totals, is_busiest)
    return (lengths.reshape(REQS), table.reshape(REQS, MAXP))


def draw_context_lengths(key, part):
    return pool_layout(key)[0]


def draw_page_table(key, part):
    return pool_layout(key)[1]


def draw_kv_pool(key, part):
    shape = (POOL_ALL, PAGE, KVH, 2 * HD)
    values = jnp.clip(jax.random.normal(jax.random.fold_in(key, 31), shape, jnp.float32), -6.0, 6.0)
    return values.astype(jnp.bfloat16)


def draw_queries(key, part):
    shape = (STEPS, REQS, HQ, HD)
    values = jnp.clip(jax.random.normal(jax.random.fold_in(key, 41), shape, jnp.float32), -6.0, 6.0)
    return values.astype(jnp.bfloat16)


def draw_residual(key, part):
    shape = (STEPS, REQS, D)
    feature = jnp.arange(D, dtype=jnp.float32) / D
    row_scale = jnp.exp(jax.random.uniform(jax.random.fold_in(key, 52), (STEPS, REQS, 1), jnp.float32, math.log(0.3), math.log(3.0)))
    col_scale = jnp.exp(jax.random.uniform(jax.random.fold_in(key, 53), (D,), jnp.float32, -0.35, 0.35))
    noise = jax.random.normal(jax.random.fold_in(key, 51), shape, jnp.float32)
    ramp = jnp.exp(math.log(0.4) + (math.log(2.0) - math.log(0.4)) * feature)
    return jnp.clip(noise * row_scale * col_scale * ramp, -16.0, 16.0).astype(jnp.bfloat16)


def level_of(stream_key, extent, shards, low, largest):
    gain = 1.0
    for axis_at, parts in shards:
        draws = jax.random.uniform(jax.random.fold_in(jax.random.fold_in(stream_key, 6), axis_at), (parts,), jnp.float32, low / len(shards), largest / len(shards))
        gain = gain * jnp.repeat(jnp.exp(draws), extent[axis_at] // parts).reshape((-1,) + (1,) * (len(extent) - 1 - axis_at))
    return gain


def deal_out(rng, own, number, rows, amount, top, limit, slope):
    order = jax.random.permutation(rng, amount)
    heavy_load, ordinary = load_shares(amount, rows * top, limit, slope, True), load_shares(amount, rows * top, limit, slope, False)
    places = jnp.arange(amount)

    def named(sizes, turn):
        used = int((sizes > 0).sum())
        fixed = max(1, used // 4)
        passed = fixed + (places - fixed + turn * (used - fixed)) % max(1, amount - fixed)
        return jnp.zeros((amount,), jnp.int32).at[order[jnp.where(places < fixed, places, passed)]].set(jnp.asarray(sizes, jnp.int32))

    sizes = jnp.where(number % 4 == 0, named(heavy_load, number // 4), named(ordinary, number - number // 4 - 1))
    mixed = jax.random.permutation(jax.random.fold_in(own, 3), amount)
    giver, sink = mixed[0:amount // 2 * 2:2], mixed[1:amount // 2 * 2:2]
    room = jnp.minimum(sizes[giver] - 1, limit - sizes[sink]) // 2
    room = jnp.where((giver == order[0]) | (sink == order[0]) | (sizes[sink] == 0), 0, jnp.maximum(room, 0))
    passed = jax.random.randint(jax.random.fold_in(own, 4), (amount // 2,), 0, 1 << 20) % (room + 1)
    sizes = sizes.at[giver].add(-passed).at[sink].add(passed)
    members = jnp.searchsorted(jnp.cumsum(sizes), jnp.arange(rows * top), side="right").astype(jnp.int32)
    table = members.reshape(top, rows).T
    table = table[jax.random.permutation(jax.random.fold_in(own, 1), rows)]
    turn = jax.random.randint(jax.random.fold_in(own, 2), (rows, 1), 0, top)
    return jnp.take_along_axis(table, (jnp.arange(top)[None, :] + turn) % top, axis=1)


def load_shares(amount, total, limit, slope, full):
    loads = [(1 << 20) // math.isqrt(standing ** slope) + 1 for standing in range(1, amount + 1)]
    largest = limit if full else min(limit, max(-(-total // amount), total * loads[0] // sum(loads)))
    least = 1 if total - largest >= amount - 1 else 0
    given, spare = [largest] + [least] * (amount - 1), total - largest - least * (amount - 1)
    while spare > 0:
        movable = [i for i in range(1, amount) if given[i] < largest] or [i for i in range(1, amount) if given[i] < limit]
        pool, budget = sum([loads[i] for i in movable]), spare
        for i in movable:
            addition = min(limit - given[i], max(1, budget * loads[i] // pool), spare)
            given[i] = given[i] + addition
            spare = spare - addition
    return np.array(given)


def gaussian(own_key, dims, scale, bound, cuts=(), kind=jnp.bfloat16):
    array = scale * jax.random.normal(own_key, dims, jnp.float32)
    if cuts:
        array = array * level_of(own_key, dims, cuts, -0.22, 0.18)
    return jnp.clip(array, -bound, bound).astype(kind)


def setup_inputs(seed: int = 0, part: int = 0) -> dict:
    arg_keys = jax.random.split(jax.random.key(seed), 13)
    part_splits = jax.random.split(jax.random.fold_in(arg_keys[12], part), 13)
    queries = draw_queries(jax.random.fold_in(jax.random.fold_in(arg_keys[12], part), 71), part)
    fresh_kv = gaussian(part_splits[1], (STEPS, REQS, KVH, 2 * HD), 1.0, 6.0, ((1, 8), (2, 2)))
    kv_pool = draw_kv_pool(jax.random.fold_in(jax.random.fold_in(arg_keys[12], part), 71), part)
    page_table = draw_page_table(jax.random.fold_in(jax.random.fold_in(arg_keys[12], part), 71), part)
    context_lengths = draw_context_lengths(jax.random.fold_in(jax.random.fold_in(arg_keys[12], part), 71), part)
    residual = draw_residual(jax.random.fold_in(jax.random.fold_in(arg_keys[12], part), 71), part)
    out_weight = gaussian(arg_keys[6], (HQ * HD, D), (HQ * HD) ** -0.5, 0.09375, ((0, 2), (1, 8)))
    norm_gain = jnp.clip(1.0 + 0.18 * jax.random.normal(arg_keys[7], (D,), jnp.float32), 0.1, 1.9)
    expert_ids_keys = jax.random.split(jax.random.fold_in(part_splits[8], 1), STEPS * REQS // REQ_DP)
    expert_ids_turns = jax.random.permutation(jax.random.fold_in(part_splits[8], 3), STEPS * REQS // REQ_DP)
    expert_ids = jax.vmap(lambda own, number: deal_out(jax.random.fold_in(part_splits[8], 2), own, number, REQ_DP, EXPERTS, TOP, CAP, 2))(expert_ids_keys, expert_ids_turns).reshape((STEPS, REQS, TOP))
    route_weights = jnp.clip(jnp.exp(math.log(1.0) - 2.3025851 * jax.random.uniform(part_splits[9], (STEPS, REQS, TOP), jnp.float32) ** level_of(part_splits[9], (STEPS, REQS, TOP), ((1, 8),), -0.2, 0.2)), 0.1, 1.0)
    gate_up = gaussian(arg_keys[10], (EXPERTS, 2, D, HID), D ** -0.5, 0.09375, ((0, 8), (2, 2)))
    down_proj = gaussian(arg_keys[11], (EXPERTS, HID, D), HID ** -0.5, 0.21875, ((0, 8), (2, 2)))
    return dict(queries=queries, fresh_kv=fresh_kv, kv_pool=kv_pool, page_table=page_table, context_lengths=context_lengths, residual=residual, out_weight=out_weight, norm_gain=norm_gain, expert_ids=expert_ids, route_weights=route_weights, gate_up=gate_up, down_proj=down_proj)


NEG = -1e+30
EPS = 1e-06
EXACT = lax.Precision.HIGHEST

def page_owners(table, lengths, pool_pages, page_len):
    pages = jnp.arange(pool_pages, dtype=jnp.int32)
    matches = table[:, :, None] == pages[None, None, :]
    ownership = jnp.any(matches, axis=1)
    slot_index = jnp.arange(table.shape[1], dtype=jnp.int32)
    position = lax.optimization_barrier(jnp.sum(jnp.where(matches, slot_index[None, :, None], 0), axis=(0, 1)))
    owner_length = lax.optimization_barrier(jnp.sum(jnp.where(ownership, lengths[:, None], 0), axis=0))
    live_count = jnp.clip(owner_length - position * page_len, 0, page_len)
    return (ownership, live_count)

def attend(query_block, fresh_block, pool_block, table_block, length_block):
    step_count, req_count, head_count, head_width = query_block.shape
    pool_pages, page_len, kv_heads, _ = pool_block.shape
    group_size = head_count // kv_heads
    score_scale = 1.0 / jnp.sqrt(jnp.float32(head_width))
    ownership, live_count = page_owners(table_block, length_block, pool_pages, page_len)
    owned_f = ownership.astype(jnp.float32)
    grouped = query_block.reshape(step_count, req_count, kv_heads, group_size, head_width).astype(jnp.float32)
    page_query = jnp.einsum('rp,srkgd->pskgd', owned_f, grouped, precision=EXACT)
    key_rows = pool_block[..., :head_width].astype(jnp.float32)
    value_rows = pool_block[..., head_width:].astype(jnp.float32)
    page_scores = jnp.einsum('pskgd,ptkd->pskgt', page_query, key_rows) * score_scale
    in_page = jnp.arange(page_len)[None, :] < live_count[:, None]
    page_scores = jnp.where(in_page[:, None, None, None, :], page_scores, NEG)
    fresh_keys = fresh_block[..., :head_width].astype(jnp.float32)
    fresh_values = fresh_block[..., head_width:].astype(jnp.float32)
    fresh_scores = jnp.einsum('srkgd,urkd->srkgu', grouped, fresh_keys) * score_scale
    causal = jnp.arange(step_count)[:, None] >= jnp.arange(step_count)[None, :]
    fresh_scores = jnp.where(causal[:, None, None, None, :], fresh_scores, NEG)
    page_best = lax.optimization_barrier(jnp.max(page_scores, axis=4))
    row_best = lax.optimization_barrier(jnp.max(jnp.where(ownership[:, :, None, None, None], page_best[None], NEG), axis=1))
    row_best = jnp.maximum(row_best, jnp.moveaxis(lax.optimization_barrier(jnp.max(fresh_scores, axis=4)), 0, 1))
    owner_best = jnp.einsum('rp,rskg->pskg', owned_f, row_best, precision=EXACT)
    page_probs = jnp.exp(page_scores - owner_best[..., None])
    page_sum = lax.optimization_barrier(jnp.sum(page_probs, axis=4))
    page_rounded = page_probs.astype(jnp.bfloat16).astype(jnp.float32)
    page_acc = jnp.einsum('pskgt,ptkd->pskgd', page_rounded, value_rows)
    denominator = jnp.einsum('rp,pskg->rskg', owned_f, page_sum, precision=EXACT)
    numerator = jnp.einsum('rp,pskgd->rskgd', owned_f, page_acc, precision=EXACT)
    fresh_probs = jnp.exp(fresh_scores - jnp.moveaxis(row_best, 1, 0)[..., None])
    denominator = denominator + jnp.moveaxis(lax.optimization_barrier(jnp.sum(fresh_probs, axis=4)), 0, 1)
    fresh_rounded = fresh_probs.astype(jnp.bfloat16).astype(jnp.float32)
    numerator = numerator + jnp.einsum('srkgu,urkd->rskgd', fresh_rounded, fresh_values)
    attended = numerator / denominator[..., None]
    attended = jnp.moveaxis(attended, 1, 0)
    return attended.reshape(step_count, req_count, head_count * head_width).astype(jnp.bfloat16)

def route_experts(normed, expert_ids, route_weights, gate_up, down_proj):
    row_total = STEPS * REQS
    blocks = expert_ids.reshape(STEPS, N_DP, REQ_DP, TOP)
    catalog = jnp.arange(EXPERTS, dtype=jnp.int32)
    named_mask = jnp.any(blocks[..., None] == catalog, axis=3).astype(jnp.int32)
    earlier = jnp.cumsum(named_mask, axis=2) - named_mask
    slot_rank = jnp.take_along_axis(earlier, blocks, axis=3)
    source = jnp.arange(N_DP, dtype=jnp.int32)[None, :, None, None]
    step_index = jnp.arange(STEPS, dtype=jnp.int32)[:, None, None, None]
    slot_keys = ((blocks * N_DP + source) * STEPS + step_index) * CAP + slot_rank
    row_index = (step_index * N_DP + source) * REQ_DP + jnp.arange(REQ_DP, dtype=jnp.int32)[None, None, :, None]
    row_index = jnp.broadcast_to(row_index, slot_keys.shape).astype(jnp.int32)
    slot_count = EXPERTS * N_DP * STEPS * CAP
    slot_rows = jnp.full((slot_count,), row_total, jnp.int32).at[slot_keys.reshape(-1)].set(row_index.reshape(-1))
    padded = jnp.concatenate([normed, jnp.zeros((1, D), normed.dtype)], axis=0)
    gathered = padded[slot_rows].reshape(EXPERTS, N_DP * STEPS * CAP, D)

    def one_expert(operands):
        expert_rows, weights_pair, weights_down = operands
        gate = jnp.dot(expert_rows, weights_pair[0], preferred_element_type=jnp.float32)
        up_value = jnp.dot(expert_rows, weights_pair[1], preferred_element_type=jnp.float32)
        activated = (jax.nn.silu(gate) * up_value).astype(jnp.bfloat16)
        return jnp.dot(activated, weights_down, preferred_element_type=jnp.float32).astype(jnp.bfloat16)
    results = lax.map(one_expert, (gathered, gate_up, down_proj)).reshape(slot_count, D)
    picked = results[slot_keys].astype(jnp.float32)
    share = route_weights.reshape(STEPS, N_DP, REQ_DP, TOP)
    share = share / lax.optimization_barrier(jnp.sum(share, axis=3, keepdims=True))
    mixture = lax.optimization_barrier(jnp.sum(share[..., None] * picked, axis=3))
    return mixture.reshape(row_total, D)

def reference(queries, fresh_kv, kv_pool, page_table, context_lengths, residual, out_weight, norm_gain, expert_ids, route_weights, gate_up, down_proj):
    query_blocks = jnp.moveaxis(queries.reshape(STEPS, N_DP, REQ_DP, HQ, HD), 1, 0)
    fresh_blocks = jnp.moveaxis(fresh_kv.reshape(STEPS, N_DP, REQ_DP, KVH, 2 * HD), 1, 0)
    pool_blocks = kv_pool.reshape(N_DP, POOL, PAGE, KVH, 2 * HD)
    table_blocks = page_table.reshape(N_DP, REQ_DP, MAXP)
    length_blocks = context_lengths.reshape(N_DP, REQ_DP)

    def per_block(operands):
        return attend(operands[0], operands[1], operands[2], operands[3], operands[4])
    attended = lax.map(per_block, (query_blocks, fresh_blocks, pool_blocks, table_blocks, length_blocks))
    attended = jnp.moveaxis(attended, 0, 1).reshape(STEPS * REQS, HQ * HD)
    projected = jnp.dot(attended, out_weight, preferred_element_type=jnp.float32)
    stream = residual.astype(jnp.float32).reshape(STEPS * REQS, D) + projected
    inverse = lax.rsqrt(lax.optimization_barrier(jnp.mean(stream * stream, axis=1)) + EPS)
    normed = (stream * inverse[:, None] * norm_gain[None, :]).astype(jnp.bfloat16)
    mixture = route_experts(normed, expert_ids, route_weights, gate_up, down_proj)
    return (stream + mixture).reshape(STEPS, REQS, D).astype(jnp.bfloat16)
```

```python
import math

import jax
import jax.numpy as jnp
from jax import lax
from jax.sharding import PartitionSpec as P

NEG = -1e30
EPS = 1e-06
EXACT = lax.Precision.HIGHEST


def page_owners(table, lengths, pool_pages, page_len):
    pages = jnp.arange(pool_pages, dtype=jnp.int32)
    matches = table[:, :, None] == pages[None, None, :]
    ownership = jnp.any(matches, axis=1)
    slot_index = jnp.arange(table.shape[1], dtype=jnp.int32)
    position = jnp.sum(jnp.where(matches, slot_index[None, :, None], 0), axis=(0, 1))
    owner_length = jnp.sum(jnp.where(ownership, lengths[:, None], 0), axis=0)
    live_count = jnp.clip(owner_length - position * page_len, 0, page_len)
    return (ownership, live_count)


def attend(query_block, fresh_block, pool_block, table_block, length_block):
    step_count, req_count, head_count, head_width = query_block.shape
    pool_pages, page_len, kv_heads, _ = pool_block.shape
    group_size = head_count // kv_heads
    score_scale = 1.0 / math.sqrt(head_width)
    ownership, live_count = page_owners(table_block, length_block, pool_pages, page_len)
    owned_f = ownership.astype(jnp.float32)
    grouped = query_block.reshape(step_count, req_count, kv_heads, group_size, head_width)
    page_query = jnp.einsum(
        "rp,srkgd->pskgd",
        ownership.astype(jnp.bfloat16),
        grouped,
        preferred_element_type=jnp.float32,
    ).astype(jnp.bfloat16)
    key_rows = pool_block[..., :head_width]
    value_rows = pool_block[..., head_width:]
    page_scores = (
        jnp.einsum("pskgd,ptkd->pskgt", page_query, key_rows, preferred_element_type=jnp.float32)
        * score_scale
    )
    in_page = jnp.arange(page_len)[None, :] < live_count[:, None]
    page_scores = jnp.where(in_page[:, None, None, None, :], page_scores, NEG)
    fresh_keys = fresh_block[..., :head_width]
    fresh_values = fresh_block[..., head_width:]
    fresh_scores = (
        jnp.einsum("srkgd,urkd->srkgu", grouped, fresh_keys, preferred_element_type=jnp.float32)
        * score_scale
    )
    causal = jnp.arange(step_count)[:, None] >= jnp.arange(step_count)[None, :]
    fresh_scores = jnp.where(causal[:, None, None, None, :], fresh_scores, NEG)
    page_best = jnp.max(page_scores, axis=4)
    row_best = jnp.max(jnp.where(ownership[:, :, None, None, None], page_best[None], NEG), axis=1)
    row_best = jnp.maximum(row_best, jnp.moveaxis(jnp.max(fresh_scores, axis=4), 0, 1))
    owner_best = jnp.einsum("rp,rskg->pskg", owned_f, row_best, precision=EXACT)
    page_probs = jnp.exp(page_scores - owner_best[..., None])
    page_sum = jnp.sum(page_probs, axis=4)
    page_acc = jnp.einsum(
        "pskgt,ptkd->pskgd",
        page_probs.astype(jnp.bfloat16),
        value_rows,
        preferred_element_type=jnp.float32,
    )
    denominator = jnp.einsum("rp,pskg->rskg", owned_f, page_sum, precision=EXACT)
    numerator = jnp.einsum("rp,pskgd->rskgd", owned_f, page_acc, precision=EXACT)
    fresh_probs = jnp.exp(fresh_scores - jnp.moveaxis(row_best, 1, 0)[..., None])
    denominator = denominator + jnp.moveaxis(jnp.sum(fresh_probs, axis=4), 0, 1)
    numerator = numerator + jnp.einsum(
        "srkgu,urkd->rskgd",
        fresh_probs.astype(jnp.bfloat16),
        fresh_values,
        preferred_element_type=jnp.float32,
    )
    attended = jnp.moveaxis(numerator / denominator[..., None], 1, 0)
    return attended.reshape(step_count, req_count, head_count * head_width).astype(jnp.bfloat16)


def exchange(value, axis, mask):
    count = lax.axis_size(axis)
    return lax.ppermute(value, axis, [(i, i ^ mask) for i in range(count)])


def reorder(blocks, index):
    blocks = list(blocks)
    for bit in range(len(blocks).bit_length() - 1):
        flip = (index >> bit) & 1 == 1
        blocks = [jnp.where(flip, blocks[j ^ (1 << bit)], blocks[j]) for j in range(len(blocks))]
    return blocks


def split_pair(value):
    high = lax.reduce_precision(value, 8, 7)
    return high.astype(jnp.bfloat16), (value - high).astype(jnp.bfloat16)


def gather_rows(rows):
    chips = lax.axis_size("dp") // 2
    mine = jnp.stack([rows] + [exchange(rows, "dp", 2 * k) for k in range(1, chips)])
    return jnp.stack([mine, exchange(mine, "dp", 1)])


def body(
    queries,
    fresh_kv,
    kv_pool,
    page_table,
    context_lengths,
    residual,
    out_weight,
    norm_gain,
    expert_ids,
    route_weights,
    gate_up,
    down_proj,
):
    bf16, f32 = jnp.bfloat16, jnp.float32
    dp_count, x_count = lax.axis_size("dp"), lax.axis_size("expert")
    dp_index, x_index = lax.axis_index("dp"), lax.axis_index("expert")
    chips = dp_count // 2
    local_experts, _, width, hidden = gate_up.shape
    expert_total = local_experts * dp_count

    share = route_weights / jnp.sum(route_weights, axis=2, keepdims=True)
    catalog = jnp.arange(expert_total, dtype=jnp.int32)
    named = expert_ids[..., None] == catalog
    routed = jnp.sum(jnp.where(named, share[..., None], 0.0), axis=2)

    attended = attend(queries, fresh_kv, kv_pool, page_table, context_lengths)
    steps, reqs, head_cols = attended.shape
    own = steps * reqs
    total = dp_count * own
    extra = -(-2 * expert_total // 128) * 128
    routed_high, routed_low = split_pair(routed.reshape(own, expert_total))
    packed = jnp.concatenate(
        [
            attended.reshape(own, head_cols),
            routed_high,
            routed_low,
            jnp.zeros((own, extra - 2 * expert_total), bf16),
        ],
        axis=1,
    )
    gathered = gather_rows(packed).reshape(total, head_cols + extra)
    routes = gathered[:, head_cols : head_cols + 2 * expert_total].astype(f32)
    routes = routes[:, :expert_total] + routes[:, expert_total:]

    columns = jnp.dot(gathered[:, :head_cols], out_weight, preferred_element_type=f32).astype(bf16)
    block = columns.shape[1]
    columns = columns.reshape(2, chips, own, block)
    paired = jnp.stack([columns[0], exchange(columns[1], "dp", 1)], axis=1)
    arrived = [paired[0]] + [exchange(paired[k], "dp", 2 * k) for k in range(1, chips)]
    blocks = [arrived[q // 2][q % 2] for q in range(dp_count)]
    per_x = dp_count // x_count
    groups = [jnp.concatenate(blocks[g * per_x : (g + 1) * per_x], axis=1) for g in range(x_count)]
    groups = reorder(groups, (dp_index // per_x) ^ x_index)
    summed = groups[0].astype(f32)
    for k in range(1, x_count):
        summed = summed + exchange(groups[k], "expert", k).astype(f32)
    summed = [summed[:, q * block : (q + 1) * block] for q in range(per_x)]
    summed = jnp.concatenate(reorder(summed, dp_index % per_x), axis=1)
    stream = residual.astype(f32).reshape(own, width) + summed

    square_high, square_low = split_pair(jnp.sum(stream * stream, axis=1, keepdims=True))
    rows = jnp.concatenate(
        [
            (stream * norm_gain[None, :]).astype(bf16),
            square_high,
            square_low,
            jnp.zeros((own, 126), bf16),
        ],
        axis=1,
    )
    rows = gather_rows(rows).reshape(total, width + 128)
    squares = rows[:, width : width + 2]
    rows = rows[:, :width]

    local = dp_index * local_experts + jnp.arange(local_experts, dtype=jnp.int32)
    local_share = jnp.sum(
        jnp.where(local[None, :, None] == catalog[None, None, :], routes[:, None, :], 0.0), axis=2
    )
    part = hidden // x_count
    inverse = None
    acts = []
    for e in range(local_experts):
        gate = jnp.dot(rows, gate_up[e, 0], preferred_element_type=f32)
        up = jnp.dot(rows, gate_up[e, 1], preferred_element_type=f32)
        gates = reorder([gate[:, k * part : (k + 1) * part] for k in range(x_count)], x_index)
        ups = reorder([up[:, k * part : (k + 1) * part] for k in range(x_count)], x_index)
        gate, up = gates[0], ups[0]
        square = jnp.sum(squares.astype(f32), axis=1)
        for k in range(1, x_count):
            sent = [gates[k].astype(bf16), ups[k].astype(bf16)]
            if e == 0:
                sent.append(squares)
            got = exchange(jnp.concatenate(sent, axis=1), "expert", k).astype(f32)
            gate = gate + got[:, :part]
            up = up + got[:, part : 2 * part]
            if e == 0:
                square = square + jnp.sum(got[:, 2 * part :], axis=1)
        if e == 0:
            inverse = lax.rsqrt(square / (width * x_count) + EPS)[:, None]
        act = jax.nn.silu(gate * inverse) * (up * inverse) * local_share[:, e : e + 1]
        act = act.astype(bf16)
        pieces = [act] + [exchange(act, "expert", k) for k in range(1, x_count)]
        acts.extend(reorder(pieces, x_index))
    activated = jnp.concatenate(acts, axis=1)
    down = down_proj.reshape(local_experts * hidden, width)
    mixed = jnp.dot(activated, down, preferred_element_type=f32)
    mixed = mixed.reshape(2, chips, own, width)
    mixed = mixed[0] + exchange(mixed[1].astype(bf16), "dp", 1).astype(f32)
    result = stream + mixed[0]
    for k in range(1, chips):
        result = result + exchange(mixed[k].astype(bf16), "dp", 2 * k).astype(f32)
    return result.reshape(steps, reqs, width).astype(bf16)


def solution(mesh):
    return jax.shard_map(
        body,
        mesh=mesh,
        in_specs=(
            P(None, ("groups", "dp"), "expert", None),
            P(None, ("groups", "dp"), "expert", None),
            P(("groups", "dp"), None, "expert", None),
            P(("groups", "dp"), None),
            P(("groups", "dp")),
            P(None, ("groups", "dp"), "expert"),
            P("expert", "dp"),
            P("expert"),
            P(None, ("groups", "dp"), None),
            P(None, ("groups", "dp"), None),
            P("dp", None, "expert", None),
            P("dp", None, "expert"),
        ),
        out_specs=P(None, ("groups", "dp"), "expert"),
        check_vma=False,
    )
```

```python
import functools
import math

import jax
import jax.numpy as jnp
from jax import lax
from jax.experimental import pallas as pl
from jax.experimental.pallas import tpu as pltpu
from jax.sharding import PartitionSpec as P

NEG = -1e30
EPS = 1e-06
EXACT = lax.Precision.HIGHEST


def page_owners(table, lengths, pool_pages, page_len):
    pages = jnp.arange(pool_pages, dtype=jnp.int32)
    matches = table[:, :, None] == pages[None, None, :]
    ownership = jnp.any(matches, axis=1)
    slot_index = jnp.arange(table.shape[1], dtype=jnp.int32)
    position = jnp.sum(jnp.where(matches, slot_index[None, :, None], 0), axis=(0, 1))
    owner_length = jnp.sum(jnp.where(ownership, lengths[:, None], 0), axis=0)
    live_count = jnp.clip(owner_length - position * page_len, 0, page_len)
    return (ownership, live_count)


def attend(query_block, fresh_block, pool_block, table_block, length_block):
    step_count, req_count, head_count, head_width = query_block.shape
    pool_pages, page_len, kv_heads, _ = pool_block.shape
    group_size = head_count // kv_heads
    score_scale = 1.0 / math.sqrt(head_width)
    ownership, live_count = page_owners(table_block, length_block, pool_pages, page_len)
    owned_f = ownership.astype(jnp.float32)
    grouped = query_block.reshape(step_count, req_count, kv_heads, group_size, head_width)
    page_query = jnp.einsum(
        "rp,srkgd->pskgd",
        ownership.astype(jnp.bfloat16),
        grouped,
        preferred_element_type=jnp.float32,
    ).astype(jnp.bfloat16)
    key_rows = pool_block[..., :head_width]
    value_rows = pool_block[..., head_width:]
    page_scores = (
        jnp.einsum("pskgd,ptkd->pskgt", page_query, key_rows, preferred_element_type=jnp.float32)
        * score_scale
    )
    in_page = jnp.arange(page_len)[None, :] < live_count[:, None]
    page_scores = jnp.where(in_page[:, None, None, None, :], page_scores, NEG)
    fresh_keys = fresh_block[..., :head_width]
    fresh_values = fresh_block[..., head_width:]
    fresh_scores = (
        jnp.einsum("srkgd,urkd->srkgu", grouped, fresh_keys, preferred_element_type=jnp.float32)
        * score_scale
    )
    causal = jnp.arange(step_count)[:, None] >= jnp.arange(step_count)[None, :]
    fresh_scores = jnp.where(causal[:, None, None, None, :], fresh_scores, NEG)
    page_best = jnp.max(page_scores, axis=4)
    row_best = jnp.max(jnp.where(ownership[:, :, None, None, None], page_best[None], NEG), axis=1)
    row_best = jnp.maximum(row_best, jnp.moveaxis(jnp.max(fresh_scores, axis=4), 0, 1))
    owner_best = jnp.einsum("rp,rskg->pskg", owned_f, row_best, precision=EXACT)
    page_probs = jnp.exp(page_scores - owner_best[..., None])
    page_sum = jnp.sum(page_probs, axis=4)
    page_acc = jnp.einsum(
        "pskgt,ptkd->pskgd",
        page_probs.astype(jnp.bfloat16),
        value_rows,
        preferred_element_type=jnp.float32,
    )
    denominator = jnp.einsum("rp,pskg->rskg", owned_f, page_sum, precision=EXACT)
    numerator = jnp.einsum("rp,pskgd->rskgd", owned_f, page_acc, precision=EXACT)
    fresh_probs = jnp.exp(fresh_scores - jnp.moveaxis(row_best, 1, 0)[..., None])
    denominator = denominator + jnp.moveaxis(jnp.sum(fresh_probs, axis=4), 0, 1)
    numerator = numerator + jnp.einsum(
        "srkgu,urkd->rskgd",
        fresh_probs.astype(jnp.bfloat16),
        fresh_values,
        preferred_element_type=jnp.float32,
    )
    attended = jnp.moveaxis(numerator / denominator[..., None], 1, 0)
    return attended.reshape(step_count, req_count, head_count * head_width).astype(jnp.bfloat16)


def attend_kernel(
    req_count, group, page_len, q_ref, code_ref, extra_ref, fresh_hbm, kv_hbm, out_ref,
    kbuf, vbuf, fkbuf, fvbuf, s_ref, acc_ref, l_ref, m_ref, ksem, vsem, fsem,
):
    f32, bf16 = jnp.float32, jnp.bfloat16
    width = q_ref.shape[2]
    blocks, columns = code_ref.shape
    tokens = columns // 2
    rows = q_ref.shape[0] * group

    def fetch(half, buf, sem, b):
        part = pl.ds(b * tokens, tokens)
        return pltpu.make_async_copy(
            kv_hbm.at[part, :, pl.ds(half * width, width)], buf.at[part], sem.at[b]
        )

    fresh_copies = [
        pltpu.make_async_copy(fresh_hbm.at[:, :, pl.ds(h * width, width)], buf, fsem.at[h])
        for h, buf in enumerate((fkbuf, fvbuf))
    ]
    for copy in fresh_copies:
        copy.start()
    lax.fori_loop(0, blocks, lambda b, c: (fetch(0, kbuf, ksem, b).start(), c)[1], 0)
    lax.fori_loop(0, blocks, lambda b, c: (fetch(1, vbuf, vsem, b).start(), c)[1], 0)

    q = q_ref[...].astype(f32)
    q2 = jnp.concatenate(
        [q[:, :group].reshape(rows, width), q[:, group:].reshape(rows, width)], axis=1
    ).astype(bf16)
    row = lax.broadcasted_iota(jnp.int32, (rows, 1), 0) // group
    row_req, row_step = row % req_count, row // req_count

    def widen(x):
        even = lax.broadcasted_iota(jnp.int32, x.shape, 0) % 2 == 0
        x = x.astype(f32)
        return jnp.concatenate(
            [jnp.where(even, x, 0.0), jnp.where(even, 0.0, x)], axis=1
        ).astype(bf16)

    def scores(keys):
        return lax.dot_general(
            q2, widen(keys), (((1,), (1,)), ((), ())), preferred_element_type=f32
        )

    for copy in fresh_copies:
        copy.wait()
    fresh = fkbuf.shape[0] * 2
    fresh_keys = fkbuf.reshape(fresh, width)[...]
    col = lax.broadcasted_iota(jnp.int32, (1, fresh), 1) // 2
    allowed = (col % req_count == row_req) & (col // req_count <= row_step)
    fresh_scores = jnp.where(allowed, scores(fresh_keys), NEG)

    m_ref[...] = jnp.full(m_ref.shape, NEG, f32)
    slot = lax.broadcasted_iota(jnp.int32, (1, columns), 1) // 2 % page_len

    def first(b, c):
        fetch(0, kbuf, ksem, b).wait()
        keys = kbuf.reshape(kbuf.shape[0] * 2, width)[pl.ds(b * columns, columns), :]
        code = code_ref[pl.ds(b, 1), :]
        owner = jnp.where(slot < (code & 31), code >> 5, -1)
        s = jnp.where(owner == row_req, scores(keys), NEG)
        s_ref[b] = s
        m = m_ref[...]
        for t in range(columns // width):
            m = jnp.maximum(m, s[:, t * width : (t + 1) * width])
        m_ref[...] = m
        return c

    lax.fori_loop(0, blocks, first, 0)

    even = lax.broadcasted_iota(jnp.int32, (1, width), 1) % 2 == 0
    even_fresh = lax.broadcasted_iota(jnp.int32, (1, fresh), 1) % 2 == 0

    def best(flag, flag_fresh):
        pool = jnp.max(jnp.where(flag, m_ref[...], NEG), axis=1, keepdims=True)
        new = jnp.max(jnp.where(flag_fresh, fresh_scores, NEG), axis=1, keepdims=True)
        return jnp.maximum(pool, new)

    best_even, best_odd = best(even, even_fresh), best(~even, ~even_fresh)
    m_ref[...] = jnp.where(even, best_even, best_odd)
    rate = math.log2(math.e) / math.sqrt(width)
    fresh_probs = jnp.exp2((fresh_scores - jnp.where(even_fresh, best_even, best_odd)) * rate)
    acc_ref[...] = jnp.dot(
        fresh_probs.astype(bf16), widen(fvbuf.reshape(fresh, width)[...]), preferred_element_type=f32
    )
    l_ref[...] = jnp.zeros(l_ref.shape, f32)

    def second(b, c):
        fetch(1, vbuf, vsem, b).wait()
        values = vbuf.reshape(vbuf.shape[0] * 2, width)[pl.ds(b * columns, columns), :]
        m = m_ref[...]
        total = l_ref[...]
        probs = []
        for t in range(columns // width):
            p = jnp.exp2((s_ref[b, :, t * width : (t + 1) * width] - m) * rate)
            total = total + p
            probs.append(p.astype(bf16))
        l_ref[...] = total
        acc_ref[...] += jnp.dot(
            jnp.concatenate(probs, axis=1), widen(values), preferred_element_type=f32
        )
        return c

    lax.fori_loop(0, blocks, second, 0)

    for h, (flag, flag_fresh) in enumerate(((even, even_fresh), (~even, ~even_fresh))):
        total = jnp.sum(jnp.where(flag, l_ref[...], 0.0), axis=1, keepdims=True)
        total = total + jnp.sum(jnp.where(flag_fresh, fresh_probs, 0.0), axis=1, keepdims=True)
        m_ref[...] = acc_ref[:, h * width : (h + 1) * width] / total
        for g in range(group):
            at = (h * group + g) * width
            out_ref[:, at : at + width] = m_ref[pl.ds(g, rows // group, stride=group), :].astype(bf16)
    out_ref[:, 2 * group * width :] = extra_ref[...]


def attend_pool(queries, fresh_kv, kv_pool, page_table, context_lengths, extra):
    step_count, req_count, head_count, head_width = queries.shape
    pool_pages, page_len, kv_heads, _ = kv_pool.shape
    group = head_count // kv_heads
    slot = jnp.arange(page_table.shape[1], dtype=jnp.int32)
    live = jnp.clip(context_lengths[:, None] - slot[None, :] * page_len, 0, page_len)
    entry = jnp.arange(req_count, dtype=jnp.int32)[:, None] * 32 + live
    pages = jnp.arange(pool_pages, dtype=jnp.int32)
    code = jnp.sum(
        jnp.where(page_table[:, :, None] == pages, entry[:, :, None], 0), axis=(0, 1)
    )
    blocks = 10
    code = jnp.repeat(code, page_len * kv_heads).reshape(blocks, -1)
    tokens = pool_pages * page_len
    rows, columns = step_count * req_count * group, tokens * 2 // blocks
    bf16, f32 = jnp.bfloat16, jnp.float32
    vmem, anyspace = pl.BlockSpec(memory_space=pltpu.VMEM), pl.BlockSpec(memory_space=pl.ANY)
    own = step_count * req_count
    return pl.pallas_call(
        functools.partial(attend_kernel, req_count, group, page_len),
        out_shape=jax.ShapeDtypeStruct((own, head_count * head_width + extra.shape[1]), bf16),
        in_specs=[vmem, vmem, vmem, anyspace, anyspace],
        out_specs=vmem,
        scratch_shapes=[
            pltpu.VMEM((tokens, 2, head_width), bf16),
            pltpu.VMEM((tokens, 2, head_width), bf16),
            pltpu.VMEM((own, 2, head_width), bf16),
            pltpu.VMEM((own, 2, head_width), bf16),
            pltpu.VMEM((blocks, rows, columns), f32),
            pltpu.VMEM((rows, 2 * head_width), f32),
            pltpu.VMEM((rows, head_width), f32),
            pltpu.VMEM((rows, head_width), f32),
            pltpu.SemaphoreType.DMA((blocks,)),
            pltpu.SemaphoreType.DMA((blocks,)),
            pltpu.SemaphoreType.DMA((2,)),
        ],
        compiler_params=pltpu.CompilerParams(vmem_limit_bytes=40 * 1024 * 1024),
        name="attend_pool",
    )(
        queries.reshape(own, head_count, head_width),
        code,
        extra,
        fresh_kv.reshape(own, kv_heads, 2 * head_width),
        kv_pool.reshape(tokens, kv_heads, 2 * head_width),
    )


def exchange(value, axis, mask):
    count = lax.axis_size(axis)
    return lax.ppermute(value, axis, [(i, i ^ mask) for i in range(count)])


def reorder(blocks, index):
    blocks = list(blocks)
    for bit in range(len(blocks).bit_length() - 1):
        flip = (index >> bit) & 1 == 1
        blocks = [jnp.where(flip, blocks[j ^ (1 << bit)], blocks[j]) for j in range(len(blocks))]
    return blocks


def split_pair(value):
    high = lax.reduce_precision(value, 8, 7)
    return high.astype(jnp.bfloat16), (value - high).astype(jnp.bfloat16)


def gather_rows(rows):
    chips = lax.axis_size("dp") // 2
    mine = jnp.stack([rows] + [exchange(rows, "dp", 2 * k) for k in range(1, chips)])
    return jnp.stack([mine, exchange(mine, "dp", 1)])


def body(
    queries,
    fresh_kv,
    kv_pool,
    page_table,
    context_lengths,
    residual,
    out_weight,
    norm_gain,
    expert_ids,
    route_weights,
    gate_up,
    down_proj,
):
    bf16, f32 = jnp.bfloat16, jnp.float32
    dp_count, x_count = lax.axis_size("dp"), lax.axis_size("expert")
    dp_index, x_index = lax.axis_index("dp"), lax.axis_index("expert")
    chips = dp_count // 2
    local_experts, _, width, hidden = gate_up.shape
    expert_total = local_experts * dp_count

    share = route_weights / jnp.sum(route_weights, axis=2, keepdims=True)
    catalog = jnp.arange(expert_total, dtype=jnp.int32)
    named = expert_ids[..., None] == catalog
    routed = jnp.sum(jnp.where(named, share[..., None], 0.0), axis=2)

    steps, reqs = queries.shape[:2]
    own = steps * reqs
    total = dp_count * own
    head_cols = queries.shape[2] * queries.shape[3]
    extra = -(-2 * expert_total // 128) * 128
    routed_high, routed_low = split_pair(routed.reshape(own, expert_total))
    routed = jnp.concatenate(
        [routed_high, routed_low, jnp.zeros((own, extra - 2 * expert_total), bf16)], axis=1
    )
    if kv_pool.shape[2] == 2:
        packed = attend_pool(queries, fresh_kv, kv_pool, page_table, context_lengths, routed)
    else:
        attended = attend(queries, fresh_kv, kv_pool, page_table, context_lengths)
        packed = jnp.concatenate([attended.reshape(own, head_cols), routed], axis=1)
    gathered = gather_rows(packed).reshape(total, head_cols + extra)
    routes = gathered[:, head_cols : head_cols + 2 * expert_total].astype(f32)
    routes = routes[:, :expert_total] + routes[:, expert_total:]

    columns = jnp.dot(gathered[:, :head_cols], out_weight, preferred_element_type=f32).astype(bf16)
    block = columns.shape[1]
    columns = columns.reshape(2, chips, own, block)
    paired = jnp.stack([columns[0], exchange(columns[1], "dp", 1)], axis=1)
    arrived = [paired[0]] + [exchange(paired[k], "dp", 2 * k) for k in range(1, chips)]
    blocks = [arrived[q // 2][q % 2] for q in range(dp_count)]
    per_x = dp_count // x_count
    groups = [jnp.concatenate(blocks[g * per_x : (g + 1) * per_x], axis=1) for g in range(x_count)]
    groups = reorder(groups, (dp_index // per_x) ^ x_index)
    summed = groups[0].astype(f32)
    for k in range(1, x_count):
        summed = summed + exchange(groups[k], "expert", k).astype(f32)
    summed = [summed[:, q * block : (q + 1) * block] for q in range(per_x)]
    summed = jnp.concatenate(reorder(summed, dp_index % per_x), axis=1)
    stream = residual.astype(f32).reshape(own, width) + summed

    square_high, square_low = split_pair(jnp.sum(stream * stream, axis=1, keepdims=True))
    rows = jnp.concatenate(
        [
            (stream * norm_gain[None, :]).astype(bf16),
            square_high,
            square_low,
            jnp.zeros((own, 126), bf16),
        ],
        axis=1,
    )
    rows = gather_rows(rows).reshape(total, width + 128)
    squares = rows[:, width : width + 2]
    rows = rows[:, :width]

    local = dp_index * local_experts + jnp.arange(local_experts, dtype=jnp.int32)
    local_share = jnp.sum(
        jnp.where(local[None, :, None] == catalog[None, None, :], routes[:, None, :], 0.0), axis=2
    )
    part = hidden // x_count
    inverse = None
    acts = []
    for e in range(local_experts):
        gate = jnp.dot(rows, gate_up[e, 0], preferred_element_type=f32)
        up = jnp.dot(rows, gate_up[e, 1], preferred_element_type=f32)
        gates = reorder([gate[:, k * part : (k + 1) * part] for k in range(x_count)], x_index)
        ups = reorder([up[:, k * part : (k + 1) * part] for k in range(x_count)], x_index)
        gate, up = gates[0], ups[0]
        square = jnp.sum(squares.astype(f32), axis=1)
        for k in range(1, x_count):
            sent = [gates[k].astype(bf16), ups[k].astype(bf16)]
            if e == 0:
                sent.append(squares)
            got = exchange(jnp.concatenate(sent, axis=1), "expert", k).astype(f32)
            gate = gate + got[:, :part]
            up = up + got[:, part : 2 * part]
            if e == 0:
                square = square + jnp.sum(got[:, 2 * part :], axis=1)
        if e == 0:
            inverse = lax.rsqrt(square / (width * x_count) + EPS)[:, None]
        act = jax.nn.silu(gate * inverse) * (up * inverse) * local_share[:, e : e + 1]
        act = act.astype(bf16)
        pieces = [act] + [exchange(act, "expert", k) for k in range(1, x_count)]
        acts.extend(reorder(pieces, x_index))
    activated = jnp.concatenate(acts, axis=1)
    down = down_proj.reshape(local_experts * hidden, width)
    mixed = jnp.dot(activated, down, preferred_element_type=f32)
    mixed = mixed.reshape(2, chips, own, width)
    mixed = mixed[0] + exchange(mixed[1].astype(bf16), "dp", 1).astype(f32)
    result = stream + mixed[0]
    for k in range(1, chips):
        result = result + exchange(mixed[k].astype(bf16), "dp", 2 * k).astype(f32)
    return result.reshape(steps, reqs, width).astype(bf16)


def solution(mesh):
    return jax.shard_map(
        body,
        mesh=mesh,
        in_specs=(
            P(None, ("groups", "dp"), "expert", None),
            P(None, ("groups", "dp"), "expert", None),
            P(("groups", "dp"), None, "expert", None),
            P(("groups", "dp"), None),
            P(("groups", "dp")),
            P(None, ("groups", "dp"), "expert"),
            P("expert", "dp"),
            P("expert"),
            P(None, ("groups", "dp"), None),
            P(None, ("groups", "dp"), None),
            P("dp", None, "expert", None),
            P("dp", None, "expert"),
        ),
        out_specs=P(None, ("groups", "dp"), "expert"),
        check_vma=False,
    )
```

```python
import functools
import math

import jax
import jax.numpy as jnp
from jax import lax
from jax.experimental import pallas as pl
from jax.experimental.pallas import tpu as pltpu
from jax.sharding import PartitionSpec as P

NEG = -1e30
EPS = 1e-06
EXACT = lax.Precision.HIGHEST


def page_owners(table, lengths, pool_pages, page_len):
    pages = jnp.arange(pool_pages, dtype=jnp.int32)
    matches = table[:, :, None] == pages[None, None, :]
    ownership = jnp.any(matches, axis=1)
    slot_index = jnp.arange(table.shape[1], dtype=jnp.int32)
    position = jnp.sum(jnp.where(matches, slot_index[None, :, None], 0), axis=(0, 1))
    owner_length = jnp.sum(jnp.where(ownership, lengths[:, None], 0), axis=0)
    live_count = jnp.clip(owner_length - position * page_len, 0, page_len)
    return (ownership, live_count)


def attend(query_block, fresh_block, pool_block, table_block, length_block):
    step_count, req_count, head_count, head_width = query_block.shape
    pool_pages, page_len, kv_heads, _ = pool_block.shape
    group_size = head_count // kv_heads
    score_scale = 1.0 / math.sqrt(head_width)
    ownership, live_count = page_owners(table_block, length_block, pool_pages, page_len)
    owned_f = ownership.astype(jnp.float32)
    grouped = query_block.reshape(step_count, req_count, kv_heads, group_size, head_width)
    page_query = jnp.einsum(
        "rp,srkgd->pskgd",
        ownership.astype(jnp.bfloat16),
        grouped,
        preferred_element_type=jnp.float32,
    ).astype(jnp.bfloat16)
    key_rows = pool_block[..., :head_width]
    value_rows = pool_block[..., head_width:]
    page_scores = (
        jnp.einsum("pskgd,ptkd->pskgt", page_query, key_rows, preferred_element_type=jnp.float32)
        * score_scale
    )
    in_page = jnp.arange(page_len)[None, :] < live_count[:, None]
    page_scores = jnp.where(in_page[:, None, None, None, :], page_scores, NEG)
    fresh_keys = fresh_block[..., :head_width]
    fresh_values = fresh_block[..., head_width:]
    fresh_scores = (
        jnp.einsum("srkgd,urkd->srkgu", grouped, fresh_keys, preferred_element_type=jnp.float32)
        * score_scale
    )
    causal = jnp.arange(step_count)[:, None] >= jnp.arange(step_count)[None, :]
    fresh_scores = jnp.where(causal[:, None, None, None, :], fresh_scores, NEG)
    page_best = jnp.max(page_scores, axis=4)
    row_best = jnp.max(jnp.where(ownership[:, :, None, None, None], page_best[None], NEG), axis=1)
    row_best = jnp.maximum(row_best, jnp.moveaxis(jnp.max(fresh_scores, axis=4), 0, 1))
    owner_best = jnp.einsum("rp,rskg->pskg", owned_f, row_best, precision=EXACT)
    page_probs = jnp.exp(page_scores - owner_best[..., None])
    page_sum = jnp.sum(page_probs, axis=4)
    page_acc = jnp.einsum(
        "pskgt,ptkd->pskgd",
        page_probs.astype(jnp.bfloat16),
        value_rows,
        preferred_element_type=jnp.float32,
    )
    denominator = jnp.einsum("rp,pskg->rskg", owned_f, page_sum, precision=EXACT)
    numerator = jnp.einsum("rp,pskgd->rskgd", owned_f, page_acc, precision=EXACT)
    fresh_probs = jnp.exp(fresh_scores - jnp.moveaxis(row_best, 1, 0)[..., None])
    denominator = denominator + jnp.moveaxis(jnp.sum(fresh_probs, axis=4), 0, 1)
    numerator = numerator + jnp.einsum(
        "srkgu,urkd->rskgd",
        fresh_probs.astype(jnp.bfloat16),
        fresh_values,
        preferred_element_type=jnp.float32,
    )
    attended = jnp.moveaxis(numerator / denominator[..., None], 1, 0)
    return attended.reshape(step_count, req_count, head_count * head_width).astype(jnp.bfloat16)


def attend_kernel(
    req_count, group, page_len, index_ref, code_ref, q_hbm, fresh_hbm, kv_hbm, gate_up_hbm, down_hbm,
    out_ref, gate_up_ref, down_ref, q_ref, kbuf, vbuf, fkbuf, fvbuf, s_ref, acc_ref, l_ref, m_ref, ksem, vsem, fsem, wsem,
):
    f32, bf16 = jnp.float32, jnp.bfloat16
    width = q_ref.shape[2]
    blocks, columns = code_ref.shape
    tokens = columns // 2
    rows = q_ref.shape[0] * group

    def fetch(half, buf, sem, b):
        part = pl.ds(b * tokens, tokens)
        return pltpu.make_async_copy(
            kv_hbm.at[part, :, pl.ds(half * width, width)], buf.at[part], sem.at[b]
        )

    fresh_copies = [
        pltpu.make_async_copy(fresh_hbm.at[:, :, pl.ds(h * width, width)], buf, fsem.at[h])
        for h, buf in enumerate((fkbuf, fvbuf))
    ]
    fresh_copies.append(pltpu.make_async_copy(q_hbm, q_ref, fsem.at[2]))
    for copy in fresh_copies:
        copy.start()
    lax.fori_loop(0, blocks, lambda b, c: (fetch(0, kbuf, ksem, b).start(), c)[1], 0)
    lax.fori_loop(0, blocks, lambda b, c: (fetch(1, vbuf, vsem, b).start(), c)[1], 0)
    weight_copies = [
        pltpu.make_async_copy(gate_up_hbm, gate_up_ref, wsem.at[0]),
        pltpu.make_async_copy(down_hbm, down_ref, wsem.at[1]),
    ]
    for copy in weight_copies:
        copy.start()
    for copy in fresh_copies:
        copy.wait()

    q = q_ref[...].astype(f32)
    q2 = jnp.concatenate(
        [q[:, :group].reshape(rows, width), q[:, group:].reshape(rows, width)], axis=1
    ).astype(bf16)
    row = lax.broadcasted_iota(jnp.int32, (rows, 1), 0) // group
    row_req, row_step = row % req_count, row // req_count

    def widen(x):
        even = lax.broadcasted_iota(jnp.int32, x.shape, 0) % 2 == 0
        x = x.astype(f32)
        return jnp.concatenate(
            [jnp.where(even, x, 0.0), jnp.where(even, 0.0, x)], axis=1
        ).astype(bf16)

    def scores(keys):
        return lax.dot_general(
            q2, widen(keys), (((1,), (1,)), ((), ())), preferred_element_type=f32
        )

    fresh = fkbuf.shape[0] * 2
    fresh_keys = fkbuf.reshape(fresh, width)[...]
    col = lax.broadcasted_iota(jnp.int32, (1, fresh), 1) // 2
    allowed = (col % req_count == row_req) & (col // req_count <= row_step)
    fresh_scores = jnp.where(allowed, scores(fresh_keys), NEG)

    m_ref[...] = jnp.full(m_ref.shape, NEG, f32)
    slot = lax.broadcasted_iota(jnp.int32, (1, columns), 1) // 2 % page_len

    def first(b, c):
        fetch(0, kbuf, ksem, b).wait()
        keys = kbuf.reshape(kbuf.shape[0] * 2, width)[pl.ds(b * columns, columns), :]
        code = code_ref[pl.ds(b, 1), :]
        owner = jnp.where(slot < (code & 31), code >> 5, -1)
        s = jnp.where(owner == row_req, scores(keys), NEG)
        s_ref[b] = s
        m = m_ref[...]
        for t in range(columns // width):
            m = jnp.maximum(m, s[:, t * width : (t + 1) * width])
        m_ref[...] = m
        return c

    lax.fori_loop(0, blocks, first, 0)

    even = lax.broadcasted_iota(jnp.int32, (1, width), 1) % 2 == 0
    even_fresh = lax.broadcasted_iota(jnp.int32, (1, fresh), 1) % 2 == 0

    def best(flag, flag_fresh):
        pool = jnp.max(jnp.where(flag, m_ref[...], NEG), axis=1, keepdims=True)
        new = jnp.max(jnp.where(flag_fresh, fresh_scores, NEG), axis=1, keepdims=True)
        return jnp.maximum(pool, new)

    best_even, best_odd = best(even, even_fresh), best(~even, ~even_fresh)
    m_ref[...] = jnp.where(even, best_even, best_odd)
    rate = math.log2(math.e) / math.sqrt(width)
    fresh_probs = jnp.exp2((fresh_scores - jnp.where(even_fresh, best_even, best_odd)) * rate)
    acc_ref[...] = jnp.dot(
        fresh_probs.astype(bf16), widen(fvbuf.reshape(fresh, width)[...]), preferred_element_type=f32
    )
    l_ref[...] = jnp.zeros(l_ref.shape, f32)

    def second(b, c):
        fetch(1, vbuf, vsem, b).wait()
        values = vbuf.reshape(vbuf.shape[0] * 2, width)[pl.ds(b * columns, columns), :]
        m = m_ref[...]
        total = l_ref[...]
        probs = []
        for t in range(columns // width):
            p = jnp.exp2((s_ref[b, :, t * width : (t + 1) * width] - m) * rate)
            total = total + p
            probs.append(p.astype(bf16))
        l_ref[...] = total
        acc_ref[...] += jnp.dot(
            jnp.concatenate(probs, axis=1), widen(values), preferred_element_type=f32
        )
        return c

    lax.fori_loop(0, blocks, second, 0)

    for h, (flag, flag_fresh) in enumerate(((even, even_fresh), (~even, ~even_fresh))):
        total = jnp.sum(jnp.where(flag, l_ref[...], 0.0), axis=1, keepdims=True)
        total = total + jnp.sum(jnp.where(flag_fresh, fresh_probs, 0.0), axis=1, keepdims=True)
        m_ref[...] = acc_ref[:, h * width : (h + 1) * width] / total
        for g in range(group):
            at = (h * group + g) * width
            out_ref[:, at : at + width] = m_ref[pl.ds(g, rows // group, stride=group), :].astype(bf16)
    for copy in weight_copies:
        copy.wait()


def attend_pool(index, queries, fresh_kv, kv_pool, page_table, context_lengths, gate_up, down_proj):
    step_count, req_count, head_count, head_width = queries.shape
    pool_pages, page_len, kv_heads, _ = kv_pool.shape
    group = head_count // kv_heads
    slot = jnp.arange(page_table.shape[1], dtype=jnp.int32)
    live = jnp.clip(context_lengths[:, None] - slot[None, :] * page_len, 0, page_len)
    entry = jnp.arange(req_count, dtype=jnp.int32)[:, None] * 32 + live
    pages = jnp.arange(pool_pages, dtype=jnp.int32)
    code = jnp.sum(
        jnp.where(page_table[:, :, None] == pages, entry[:, :, None], 0), axis=(0, 1)
    )
    blocks = 10
    code = jnp.repeat(code, page_len * kv_heads).reshape(blocks, -1)
    tokens = pool_pages * page_len
    rows, columns = step_count * req_count * group, tokens * 2 // blocks
    bf16, f32 = jnp.bfloat16, jnp.float32
    vmem, hbm = pl.BlockSpec(memory_space=pltpu.VMEM), pl.BlockSpec(memory_space=pltpu.HBM)
    own = step_count * req_count
    return pl.pallas_call(
        functools.partial(attend_kernel, req_count, group, page_len),
        out_shape=(
            jax.ShapeDtypeStruct((own, head_count * head_width), bf16),
            pltpu.VMEM(gate_up.shape, bf16),
            pltpu.VMEM(down_proj.shape, bf16),
        ),
        in_specs=[pl.BlockSpec(memory_space=pltpu.SMEM), vmem, hbm, hbm, hbm, hbm, hbm],
        out_specs=(vmem, vmem, vmem),
        scratch_shapes=[
            pltpu.VMEM((own, head_count, head_width), bf16),
            pltpu.VMEM((tokens, 2, head_width), bf16),
            pltpu.VMEM((tokens, 2, head_width), bf16),
            pltpu.VMEM((own, 2, head_width), bf16),
            pltpu.VMEM((own, 2, head_width), bf16),
            pltpu.VMEM((blocks, rows, columns), f32),
            pltpu.VMEM((rows, 2 * head_width), f32),
            pltpu.VMEM((rows, head_width), f32),
            pltpu.VMEM((rows, head_width), f32),
            pltpu.SemaphoreType.DMA((blocks,)),
            pltpu.SemaphoreType.DMA((blocks,)),
            pltpu.SemaphoreType.DMA((3,)),
            pltpu.SemaphoreType.DMA((2,)),
        ],
        compiler_params=pltpu.CompilerParams(vmem_limit_bytes=24 * 1024 * 1024),
        name="attend_pool",
    )(
        index,
        code,
        *[
            pltpu.with_memory_space_constraint(value, pltpu.HBM)
            for value in (
                queries.reshape(own, head_count, head_width),
                fresh_kv.reshape(own, kv_heads, 2 * head_width),
                kv_pool.reshape(tokens, kv_heads, 2 * head_width),
                gate_up,
                down_proj,
            )
        ],
    )


def exchange(value, axis, mask):
    count = lax.axis_size(axis)
    return lax.ppermute(value, axis, [(i, i ^ mask) for i in range(count)])


def reorder(blocks, index, low=0):
    blocks = list(blocks)
    for bit in range(low, len(blocks).bit_length() - 1):
        flip = (index >> bit) & 1 == 1
        blocks = [jnp.where(flip, blocks[j ^ (1 << bit)], blocks[j]) for j in range(len(blocks))]
    return blocks


def split_pair(value):
    high = lax.reduce_precision(value, 8, 7)
    return high.astype(jnp.bfloat16), (value - high).astype(jnp.bfloat16)


def where_am_i(index_ref):
    return index_ref[0], index_ref[1]


def project_kernel(pieces, index_ref, *refs):
    weight_ref, keep_ref, send_ref = refs[2 * pieces :]
    dp_index, x_index = where_am_i(index_ref)
    rows = jnp.concatenate([ref[...] for ref in refs[: 2 * pieces]], axis=0)
    near = pieces // 2
    value = jnp.dot(rows, weight_ref[...], preferred_element_type=jnp.float32)
    own = rows.shape[0] // (2 * pieces)
    stay = (dp_index // 2) // near == x_index
    for at, ref in ((0, keep_ref), (pieces, send_ref)):
        blocks = [value[(at + k) * own : (at + k + 1) * own] for k in range(pieces)]
        for k in range(pieces):
            ref[k] = jnp.where(stay, blocks[k], blocks[k ^ near]).astype(jnp.bfloat16)


def pair_kernel(keep_ref, got_ref, *outs):
    block = keep_ref.shape[2]
    for k, out in enumerate(outs):
        out[:, :block] = keep_ref[k]
        out[:, block:] = got_ref[k]


def stream_kernel(pieces, experts, index_ref, *refs):
    f32, bf16 = jnp.float32, jnp.bfloat16
    gots = refs[:pieces]
    residual_ref, gain_ref, ids_ref, weight_ref, stream_ref, rows_ref = refs[pieces:]
    dp_index, _ = where_am_i(index_ref)
    near = pieces // 2
    width = stream_ref.shape[1]
    extra = rows_ref.shape[1] - width
    sums = [gots[k][...].astype(f32) + gots[k + near][...].astype(f32) for k in range(near)]
    sums = reorder(sums, (dp_index // 2) % near)
    block = sums[0].shape[1] // 2
    at = 0
    square = 0.0
    for both in sums:
        for part in reorder([both[:, :block], both[:, block:]], dp_index % 2):
            cut = slice(at, at + block)
            value = part + residual_ref[:, cut].astype(f32)
            stream_ref[:, cut] = value
            rows_ref[:, cut] = (value * gain_ref[:, cut]).astype(bf16)
            square = square + jnp.sum(value * value, axis=1, keepdims=True)
            at += block
    column = lax.broadcasted_iota(jnp.int32, (experts, extra), 1) - 2
    expert = lax.broadcasted_iota(jnp.int32, (experts, extra), 0)
    routes = []
    for step in range(ids_ref.shape[0]):
        ids, weights = ids_ref[step], weight_ref[step]
        share = weights / jnp.sum(weights, axis=0, keepdims=True)
        label = lax.broadcasted_iota(jnp.int32, (experts, ids.shape[1]), 0)
        table = jnp.zeros(label.shape, f32)
        for k in range(ids.shape[0]):
            table = table + jnp.where(label == ids[k : k + 1], share[k : k + 1], 0.0)
        high = table.astype(bf16)
        low = (table - high.astype(f32)).astype(bf16)
        spread = 0.0
        for value, shift in ((high, 0), (low, experts)):
            chosen = jnp.where(column == expert + shift, 1.0, 0.0).astype(bf16)
            spread = spread + lax.dot_general(
                value, chosen, (((0,), (0,)), ((), ())), preferred_element_type=f32
            )
        routes.append(spread)
    routes = jnp.concatenate(routes, axis=0)
    high = square.astype(bf16).astype(f32)
    lane = lax.broadcasted_iota(jnp.int32, routes.shape, 1)
    routes = jnp.where(lane == 0, high, jnp.where(lane == 1, square - high, routes))
    rows_ref[:, width:] = routes.astype(bf16)


def gate_up_kernel(pieces, index_ref, *refs):
    weight_ref, keep_ref, send_ref, own_ref = refs[pieces:]
    local_experts, _, width, hidden = weight_ref.shape
    part = hidden // 2
    first = index_ref[1] == 0
    rows = jnp.concatenate([ref[:, :width] for ref in refs[:pieces]], axis=0)
    for e in range(local_experts):
        for side in range(2):
            at = 2 * e + side
            value = jnp.dot(rows, weight_ref[e, side], preferred_element_type=jnp.float32)
            keep_ref[at] = jnp.where(first, value[:, :part], value[:, part:])
            send = jnp.where(first, value[:, part:], value[:, :part])
            send_ref[:, at * part : (at + 1) * part] = send.astype(jnp.bfloat16)
    extra = jnp.concatenate([ref[:, width:] for ref in refs[:pieces]], axis=0)
    own_ref[...] = extra
    send_ref[:, 2 * local_experts * part :] = extra


def act_kernel(local_experts, experts, width, index_ref, keep_ref, got_ref, own_ref, out_ref):
    f32 = jnp.float32
    part = keep_ref.shape[2]
    own = own_ref[...].astype(f32)
    lane = lax.broadcasted_iota(jnp.int32, own.shape, 1)
    other = got_ref[:, 2 * local_experts * part :].astype(f32)
    square = jnp.sum(jnp.where(lane < 2, own + other, 0.0), axis=1, keepdims=True)
    inverse = lax.rsqrt(square / width + EPS)
    for e in range(local_experts):
        column = 2 + index_ref[0] * local_experts + e
        chosen = (lane == column) | (lane == column + experts)
        share = jnp.sum(jnp.where(chosen, own, 0.0), axis=1, keepdims=True)
        gate = keep_ref[2 * e] + got_ref[:, 2 * e * part : (2 * e + 1) * part].astype(f32)
        up = keep_ref[2 * e + 1] + got_ref[:, (2 * e + 1) * part : (2 * e + 2) * part].astype(f32)
        gate = gate * inverse
        act = gate / (1.0 + jnp.exp(-gate)) * (up * inverse) * share
        out_ref[:, e * part : (e + 1) * part] = act.astype(jnp.bfloat16)


def down_kernel(index_ref, act_ref, got_ref, weight_ref, keep_ref, send_ref):
    local_experts, hidden, width = weight_ref.shape
    part = hidden // 2
    half = keep_ref.shape[0]
    first = index_ref[1] == 0
    acts = []
    for e in range(local_experts):
        own = act_ref[:, e * part : (e + 1) * part]
        got = got_ref[:, e * part : (e + 1) * part]
        acts += [jnp.where(first, own, got), jnp.where(first, got, own)]
    acts = jnp.concatenate(acts, axis=1)
    step = 512
    for at in range(0, width, step):
        value = jnp.zeros((acts.shape[0], step), jnp.float32)
        for e in range(local_experts):
            value = value + jnp.dot(
                acts[:, e * hidden : (e + 1) * hidden],
                weight_ref[e, :, at : at + step],
                preferred_element_type=jnp.float32,
            )
        keep_ref[:, at : at + step] = value[:half]
        send_ref[:, at : at + step] = value[half:].astype(jnp.bfloat16)


def fold_kernel(keep_ref, got_ref, *outs):
    own = outs[0].shape[0]
    for k, out in enumerate(outs):
        cut = slice(k * own, (k + 1) * own)
        value = keep_ref[cut] + got_ref[cut].astype(jnp.float32)
        out[...] = value.astype(out.dtype)


def small_call(kernel, name, outs, *args, index=None, flops=0, limit=8):
    vmem, smem = pl.BlockSpec(memory_space=pltpu.VMEM), pl.BlockSpec(memory_space=pltpu.SMEM)
    specs = [vmem] * len(args)
    if index is not None:
        specs, args = [smem] + specs, (index,) + args
    return pl.pallas_call(
        kernel,
        out_shape=tuple(jax.ShapeDtypeStruct(shape, dtype) for shape, dtype in outs),
        in_specs=specs,
        out_specs=(vmem,) * len(outs),
        compiler_params=pltpu.CompilerParams(vmem_limit_bytes=limit * 1024 * 1024),
        cost_estimate=pl.CostEstimate(flops=flops, bytes_accessed=0, transcendentals=0)
        if flops
        else None,
        name=name,
    )(*args)


def expert_chunk(rows, x_index, dp_index, gate_up, down_proj, expert_total):
    bf16, f32 = jnp.bfloat16, jnp.float32
    x_count = lax.axis_size("expert")
    local_experts, _, width, hidden = gate_up.shape
    part = hidden // x_count
    own = rows[:, width:]
    rows = rows[:, :width]
    routes = own[:, 2 : 2 + 2 * expert_total].astype(f32)
    routes = routes[:, :expert_total] + routes[:, expert_total:]
    share = lax.dynamic_slice_in_dim(routes, dp_index * local_experts, local_experts, axis=1)
    products = [
        jnp.dot(rows, gate_up[e, s], preferred_element_type=f32)
        for e in range(local_experts)
        for s in range(2)
    ]
    parts = [
        reorder([p[:, k * part : (k + 1) * part] for k in range(x_count)], x_index) for p in products
    ]
    sums = [p[0] for p in parts]
    square = jnp.sum(own[:, :2].astype(f32), axis=1)
    for k in range(1, x_count):
        sent = jnp.concatenate([p[k].astype(bf16) for p in parts] + [own[:, :2]], axis=1)
        got = exchange(sent, "expert", k).astype(f32)
        sums = [s + got[:, i * part : (i + 1) * part] for i, s in enumerate(sums)]
        square = square + jnp.sum(got[:, len(sums) * part :], axis=1)
    inverse = lax.rsqrt(square / (width * x_count) + EPS)[:, None]
    total = 0.0
    for e in range(local_experts):
        gate, up = sums[2 * e] * inverse, sums[2 * e + 1] * inverse
        act = (jax.nn.silu(gate) * up * share[:, e : e + 1]).astype(bf16)
        pieces = [act] + [exchange(act, "expert", k) for k in range(1, x_count)]
        act = jnp.concatenate(reorder(pieces, x_index), axis=1)
        total = total + jnp.dot(act, down_proj[e], preferred_element_type=f32)
    half = total.shape[0] // 2
    return total[:half], total[half:].astype(bf16)


def body_plain(
    queries,
    fresh_kv,
    kv_pool,
    page_table,
    context_lengths,
    residual,
    out_weight,
    norm_gain,
    expert_ids,
    route_weights,
    gate_up,
    down_proj,
):
    bf16, f32 = jnp.bfloat16, jnp.float32
    dp_count, x_count = lax.axis_size("dp"), lax.axis_size("expert")
    dp_index, x_index = lax.axis_index("dp"), lax.axis_index("expert")
    chips = dp_count // 2
    chip_index, core_index = dp_index // 2, dp_index % 2
    local_experts, _, width, hidden = gate_up.shape
    expert_total = local_experts * dp_count
    steps, reqs = queries.shape[:2]
    own = steps * reqs

    attended = attend(queries, fresh_kv, kv_pool, page_table, context_lengths)
    attended = attended.reshape(own, attended.shape[2])
    mine = jnp.stack([attended] + [exchange(attended, "dp", 2 * k) for k in range(1, chips)])
    gathered = jnp.stack([mine, exchange(mine, "dp", 1)])
    gathered = gathered.reshape(dp_count * own, attended.shape[1])

    columns = jnp.dot(gathered, out_weight, preferred_element_type=f32).astype(bf16)
    block = columns.shape[1]
    columns = columns.reshape(2, chips, own, block)
    swapped = exchange(columns[1], "dp", 1)
    paired = [jnp.concatenate([columns[0, k], swapped[k]], axis=1) for k in range(chips)]
    near = chips // x_count
    low = near.bit_length() - 1
    paired = reorder(paired, ((chip_index // near) ^ x_index) * near, low)
    parts = [0.0] * near
    for k in range(chips):
        moves = []
        for z in range(chips):
            for c in range(2):
                for x in range(x_count):
                    away = (z // near) ^ x
                    there = z ^ k ^ (away * near)
                    moves.append(((2 * z + c) * x_count + x, (2 * there + c) * x_count + z // near))
        got = lax.ppermute(paired[k], ("dp", "expert"), moves).astype(f32)
        parts[k % near] = parts[k % near] + got
    parts = [
        reorder([p[:, c * block : (c + 1) * block] for c in range(2)], core_index)
        for p in reorder(parts, chip_index % near)
    ]
    stream = jnp.concatenate([b for pair in parts for b in pair], axis=1)
    stream = stream + residual.astype(f32).reshape(own, width)

    share = route_weights / jnp.sum(route_weights, axis=2, keepdims=True)
    catalog = jnp.arange(expert_total, dtype=jnp.int32)
    named = expert_ids[..., None] == catalog
    routed = jnp.sum(jnp.where(named, share[..., None], 0.0), axis=2)
    routed_high, routed_low = split_pair(routed.reshape(own, expert_total))
    square_high, square_low = split_pair(jnp.sum(stream * stream, axis=1, keepdims=True))
    extra = -(-(2 * expert_total + 2) // 128) * 128
    rows = jnp.concatenate(
        [
            (stream * norm_gain[None, :]).astype(bf16),
            square_high,
            square_low,
            routed_high,
            routed_low,
            jnp.zeros((own, extra - 2 * expert_total - 2), bf16),
        ],
        axis=1,
    )
    from_chip = [rows] + [exchange(rows, "dp", 2 * k) for k in range(1, chips)]
    result = stream
    for chunk in (range(chips // 2, chips), range(chips // 2)):
        mine = jnp.concatenate([from_chip[k] for k in chunk], axis=0)
        taken = jnp.concatenate([mine, exchange(mine, "dp", 1)], axis=0)
        keep, send = expert_chunk(taken, x_index, dp_index, gate_up, down_proj, expert_total)
        keep = keep + exchange(send, "dp", 1).astype(f32)
        for i, k in enumerate(chunk):
            piece = keep[i * own : (i + 1) * own]
            if k > 0:
                piece = exchange(piece.astype(bf16), "dp", 2 * k).astype(f32)
            result = result + piece
    return result.reshape(steps, reqs, width).astype(bf16)


def body_fast(
    queries,
    fresh_kv,
    kv_pool,
    page_table,
    context_lengths,
    residual,
    out_weight,
    norm_gain,
    expert_ids,
    route_weights,
    gate_up,
    down_proj,
):
    bf16, f32 = jnp.bfloat16, jnp.float32
    dp_count, x_count = lax.axis_size("dp"), lax.axis_size("expert")
    dp_index, x_index = lax.axis_index("dp"), lax.axis_index("expert")
    index = jnp.stack([dp_index, x_index]).astype(jnp.int32)
    chips = dp_count // 2
    local_experts, _, width, hidden = gate_up.shape
    part = hidden // 2
    expert_total = local_experts * dp_count
    steps, reqs = queries.shape[:2]
    own = steps * reqs

    attended, gate_up, down_proj = attend_pool(
        index, queries, fresh_kv, kv_pool, page_table, context_lengths, gate_up, down_proj
    )
    head_cols = attended.shape[1]
    mine = [attended] + [exchange(attended, "dp", 2 * k) for k in range(1, chips)]
    mine = mine + [exchange(piece, "dp", 1) for piece in mine]
    block = out_weight.shape[1]
    keep, send = small_call(
        functools.partial(project_kernel, chips),
        "project",
        [((chips, own, block), bf16)] * 2,
        *mine,
        out_weight,
        index=index,
        flops=2 * dp_count * own * head_cols * block,
    )
    paired = small_call(
        pair_kernel, "pair", [((own, 2 * block), bf16)] * chips, keep, exchange(send, "dp", 1)
    )
    near = chips // x_count
    arrived = []
    for k in range(chips):
        moves = []
        for z in range(chips):
            for c in range(2):
                for x in range(x_count):
                    away = (z // near) ^ x
                    there = z ^ k ^ (away * near)
                    moves.append(((2 * z + c) * x_count + x, (2 * there + c) * x_count + z // near))
        arrived.append(lax.ppermute(paired[k], ("dp", "expert"), moves))

    extra = -(-(2 * expert_total + 2) // 128) * 128
    stream, rows = small_call(
        functools.partial(stream_kernel, chips, expert_total),
        "stream",
        [((own, width), f32), ((own, width + extra), bf16)],
        *arrived,
        residual.reshape(own, width),
        norm_gain.reshape(1, width),
        jnp.swapaxes(expert_ids, 1, 2),
        jnp.swapaxes(route_weights, 1, 2),
        index=index,
    )
    from_chip = [rows] + [exchange(rows, "dp", 2 * k) for k in range(1, chips)]
    result = stream
    for chunk in (range(chips // 2, chips), range(chips // 2)):
        pieces = [from_chip[k] for k in chunk]
        pieces = pieces + [exchange(piece, "dp", 1) for piece in pieces]
        count = len(pieces) * own
        keep, send, extras = small_call(
            functools.partial(gate_up_kernel, len(pieces)),
            "gate_up",
            [
                ((2 * local_experts, count, part), f32),
                ((count, 2 * local_experts * part + extra), bf16),
                ((count, extra), bf16),
            ],
            *pieces,
            gate_up,
            index=index,
            flops=4 * count * width * hidden * local_experts,
        )
        (act,) = small_call(
            functools.partial(act_kernel, local_experts, expert_total, x_count * width),
            "act",
            [((count, local_experts * part), bf16)],
            keep,
            exchange(send, "expert", 1),
            extras,
            index=index,
        )
        keep, send = small_call(
            down_kernel,
            "down",
            [((count // 2, width), f32), ((count // 2, width), bf16)],
            act,
            exchange(act, "expert", 1),
            down_proj,
            index=index,
            flops=2 * count * width * hidden * local_experts,
        )
        folded = small_call(
            fold_kernel,
            "fold",
            [((own, width), bf16 if k else f32) for k in chunk],
            keep,
            exchange(send, "dp", 1),
        )
        for k, piece in zip(chunk, folded):
            if k > 0:
                piece = exchange(piece, "dp", 2 * k).astype(f32)
            result = result + piece
    return result.reshape(steps, reqs, width).astype(bf16)


def body(*args):
    fast = (
        args[2].shape[2] == 2
        and lax.axis_size("expert") == 2
        and lax.axis_size("dp") >= 4
        and args[10].shape[3] % 256 == 0
        and args[10].shape[2] % 512 == 0
    )
    return (body_fast if fast else body_plain)(*args)


def solution(mesh):
    return jax.shard_map(
        body,
        mesh=mesh,
        in_specs=(
            P(None, ("groups", "dp"), "expert", None),
            P(None, ("groups", "dp"), "expert", None),
            P(("groups", "dp"), None, "expert", None),
            P(("groups", "dp"), None),
            P(("groups", "dp")),
            P(None, ("groups", "dp"), "expert"),
            P("expert", "dp"),
            P("expert"),
            P(None, ("groups", "dp"), None),
            P(None, ("groups", "dp"), None),
            P("dp", None, "expert", None),
            P("dp", None, "expert"),
        ),
        out_specs=P(None, ("groups", "dp"), "expert"),
        check_vma=False,
    )
```

```python
import functools
import math

import jax
import jax.numpy as jnp
from jax import lax
from jax.experimental import pallas as pl
from jax.experimental.pallas import tpu as pltpu

from jax.sharding import PartitionSpec as P

NEG = -1e30
EPS = 1e-06
EXACT = lax.Precision.HIGHEST


def page_owners(table, lengths, pool_pages, page_len):
    pages = jnp.arange(pool_pages, dtype=jnp.int32)
    matches = table[:, :, None] == pages[None, None, :]
    ownership = jnp.any(matches, axis=1)
    slot_index = jnp.arange(table.shape[1], dtype=jnp.int32)
    position = jnp.sum(jnp.where(matches, slot_index[None, :, None], 0), axis=(0, 1))
    owner_length = jnp.sum(jnp.where(ownership, lengths[:, None], 0), axis=0)
    live_count = jnp.clip(owner_length - position * page_len, 0, page_len)
    return (ownership, live_count)


def attend(query_block, fresh_block, pool_block, table_block, length_block):
    step_count, req_count, head_count, head_width = query_block.shape
    pool_pages, page_len, kv_heads, _ = pool_block.shape
    group_size = head_count // kv_heads
    score_scale = 1.0 / math.sqrt(head_width)
    ownership, live_count = page_owners(table_block, length_block, pool_pages, page_len)
    owned_f = ownership.astype(jnp.float32)
    grouped = query_block.reshape(step_count, req_count, kv_heads, group_size, head_width)
    page_query = jnp.einsum(
        "rp,srkgd->pskgd",
        ownership.astype(jnp.bfloat16),
        grouped,
        preferred_element_type=jnp.float32,
    ).astype(jnp.bfloat16)
    key_rows = pool_block[..., :head_width]
    value_rows = pool_block[..., head_width:]
    page_scores = (
        jnp.einsum("pskgd,ptkd->pskgt", page_query, key_rows, preferred_element_type=jnp.float32)
        * score_scale
    )
    in_page = jnp.arange(page_len)[None, :] < live_count[:, None]
    page_scores = jnp.where(in_page[:, None, None, None, :], page_scores, NEG)
    fresh_keys = fresh_block[..., :head_width]
    fresh_values = fresh_block[..., head_width:]
    fresh_scores = (
        jnp.einsum("srkgd,urkd->srkgu", grouped, fresh_keys, preferred_element_type=jnp.float32)
        * score_scale
    )
    causal = jnp.arange(step_count)[:, None] >= jnp.arange(step_count)[None, :]
    fresh_scores = jnp.where(causal[:, None, None, None, :], fresh_scores, NEG)
    page_best = jnp.max(page_scores, axis=4)
    row_best = jnp.max(jnp.where(ownership[:, :, None, None, None], page_best[None], NEG), axis=1)
    row_best = jnp.maximum(row_best, jnp.moveaxis(jnp.max(fresh_scores, axis=4), 0, 1))
    owner_best = jnp.einsum("rp,rskg->pskg", owned_f, row_best, precision=EXACT)
    page_probs = jnp.exp(page_scores - owner_best[..., None])
    page_sum = jnp.sum(page_probs, axis=4)
    page_acc = jnp.einsum(
        "pskgt,ptkd->pskgd",
        page_probs.astype(jnp.bfloat16),
        value_rows,
        preferred_element_type=jnp.float32,
    )
    denominator = jnp.einsum("rp,pskg->rskg", owned_f, page_sum, precision=EXACT)
    numerator = jnp.einsum("rp,pskgd->rskgd", owned_f, page_acc, precision=EXACT)
    fresh_probs = jnp.exp(fresh_scores - jnp.moveaxis(row_best, 1, 0)[..., None])
    denominator = denominator + jnp.moveaxis(jnp.sum(fresh_probs, axis=4), 0, 1)
    numerator = numerator + jnp.einsum(
        "srkgu,urkd->rskgd",
        fresh_probs.astype(jnp.bfloat16),
        fresh_values,
        preferred_element_type=jnp.float32,
    )
    attended = jnp.moveaxis(numerator / denominator[..., None], 1, 0)
    return attended.reshape(step_count, req_count, head_count * head_width).astype(jnp.bfloat16)


def attend_kernel(
    req_count, group, page_len, blocks, index_ref, table_ref, length_ref, q_hbm, fresh_hbm, kv_hbm, gate_up_hbm, down_hbm,
    out_ref, gate_up_ref, down_ref, q_ref, kbuf, vbuf, fkbuf, fvbuf, s_ref, acc_ref, l_ref, m_ref, code_ref, ksem, vsem, fsem, wsem,
):
    f32, bf16 = jnp.float32, jnp.bfloat16
    width = q_ref.shape[2]
    tokens = kbuf.shape[0] // blocks
    columns = 2 * tokens
    pages = tokens // page_len
    rows = q_ref.shape[0] * group

    def fetch(half, buf, sem, b):
        part = pl.ds(b * tokens, tokens)
        return pltpu.make_async_copy(
            kv_hbm.at[part, :, pl.ds(half * width, width)], buf.at[part], sem.at[b]
        )

    fresh_copies = [
        pltpu.make_async_copy(fresh_hbm.at[:, :, pl.ds(h * width, width)], buf, fsem.at[h])
        for h, buf in enumerate((fkbuf, fvbuf))
    ]
    fresh_copies.append(pltpu.make_async_copy(q_hbm, q_ref, fsem.at[2]))
    for copy in fresh_copies:
        copy.start()
    lax.fori_loop(0, blocks, lambda b, c: (fetch(0, kbuf, ksem, b).start(), c)[1], 0)
    lax.fori_loop(0, blocks, lambda b, c: (fetch(1, vbuf, vsem, b).start(), c)[1], 0)
    weight_copies = [
        pltpu.make_async_copy(gate_up_hbm, gate_up_ref, wsem.at[0]),
        pltpu.make_async_copy(down_hbm, down_ref, wsem.at[1]),
    ]
    for copy in weight_copies:
        copy.start()

    def clear(p, c):
        code_ref[p] = 0
        return c

    lax.fori_loop(0, blocks * pages, clear, 0, unroll=16)
    for r in range(req_count):
        length = length_ref[r]

        def put(j, c, r=r, length=length):
            code_ref[table_ref[r, j]] = r * 32 + jnp.minimum(length - j * page_len, page_len)
            return c

        count = (length + page_len - 1) // page_len

        def four(i, c, r=r, length=length):
            spots = [table_ref[r, 4 * i + k] for k in range(4)]
            for k, spot in enumerate(spots):
                code_ref[spot] = r * 32 + jnp.minimum(length - (4 * i + k) * page_len, page_len)
            return c

        lax.fori_loop(0, count // 4, four, 0)
        lax.fori_loop(count // 4 * 4, count, put, 0)
    lane_page = lax.broadcasted_iota(jnp.int32, (1, width), 1) // (2 * page_len)
    per_tile = width // (2 * page_len)

    def codes(b):
        tiles = []
        for t in range(columns // width):
            at = b * pages + t * per_tile
            tile = jnp.zeros((1, width), jnp.int32)
            for i in range(per_tile):
                tile = jnp.where(lane_page == i, code_ref[at + i], tile)
            tiles.append(tile)
        return jnp.concatenate(tiles, axis=1)

    for copy in fresh_copies:
        copy.wait()

    q = q_ref[...].astype(f32)
    q2 = jnp.concatenate(
        [q[:, :group].reshape(rows, width), q[:, group:].reshape(rows, width)], axis=1
    ).astype(bf16)
    row = lax.broadcasted_iota(jnp.int32, (rows, 1), 0) // group
    row_req, row_step = row % req_count, row // req_count

    def widen(x):
        even = lax.broadcasted_iota(jnp.int32, x.shape, 0) % 2 == 0
        x = x.astype(f32)
        return jnp.concatenate(
            [jnp.where(even, x, 0.0), jnp.where(even, 0.0, x)], axis=1
        ).astype(bf16)

    def scores(keys):
        flat = keys.T.astype(f32)
        even = lax.broadcasted_iota(jnp.int32, (1, keys.shape[0]), 1) % 2 == 0
        both = jnp.concatenate([jnp.where(even, flat, 0.0), jnp.where(even, 0.0, flat)], axis=0)
        return jnp.dot(q2, both.astype(bf16), preferred_element_type=f32)

    fresh = fkbuf.shape[0] * 2
    fresh_keys = fkbuf.reshape(fresh, width)[...]
    col = lax.broadcasted_iota(jnp.int32, (1, fresh), 1) // 2
    allowed = (col % req_count == row_req) & (col // req_count <= row_step)
    fresh_scores = jnp.where(allowed, scores(fresh_keys), NEG)

    m_ref[...] = jnp.full(m_ref.shape, NEG, f32)
    slot = lax.broadcasted_iota(jnp.int32, (1, columns), 1) // 2 % page_len

    def first(b, c):
        fetch(0, kbuf, ksem, b).wait()
        keys = kbuf.reshape(kbuf.shape[0] * 2, width)[pl.ds(b * columns, columns), :]
        code = codes(b)
        owner = jnp.where(slot < (code & 31), code >> 5, -1)
        s = jnp.where(owner == row_req, scores(keys), NEG)
        s_ref[b] = s
        m = m_ref[...]
        for t in range(columns // width):
            m = jnp.maximum(m, s[:, t * width : (t + 1) * width])
        m_ref[...] = m
        return c

    lax.fori_loop(0, blocks, first, 0)

    even = lax.broadcasted_iota(jnp.int32, (1, width), 1) % 2 == 0
    even_fresh = lax.broadcasted_iota(jnp.int32, (1, fresh), 1) % 2 == 0

    def best(flag, flag_fresh):
        pool = jnp.max(jnp.where(flag, m_ref[...], NEG), axis=1, keepdims=True)
        new = jnp.max(jnp.where(flag_fresh, fresh_scores, NEG), axis=1, keepdims=True)
        return jnp.maximum(pool, new)

    best_even, best_odd = best(even, even_fresh), best(~even, ~even_fresh)
    m_ref[...] = jnp.where(even, best_even, best_odd)
    rate = math.log2(math.e) / math.sqrt(width)
    fresh_probs = jnp.exp2((fresh_scores - jnp.where(even_fresh, best_even, best_odd)) * rate)
    acc_ref[...] = jnp.dot(
        fresh_probs.astype(bf16), widen(fvbuf.reshape(fresh, width)[...]), preferred_element_type=f32
    )
    l_ref[...] = jnp.zeros(l_ref.shape, f32)

    def second(b, c):
        fetch(1, vbuf, vsem, b).wait()
        values = vbuf.reshape(vbuf.shape[0] * 2, width)[pl.ds(b * columns, columns), :]
        m = m_ref[...]
        total = l_ref[...]
        probs = []
        for t in range(columns // width):
            p = jnp.exp2((s_ref[b, :, t * width : (t + 1) * width] - m) * rate)
            total = total + p
            probs.append(p.astype(bf16))
        l_ref[...] = total
        acc_ref[...] += jnp.dot(
            jnp.concatenate(probs, axis=1), widen(values), preferred_element_type=f32
        )
        return c

    lax.fori_loop(0, blocks, second, 0)

    for h, (flag, flag_fresh) in enumerate(((even, even_fresh), (~even, ~even_fresh))):
        total = jnp.sum(jnp.where(flag, l_ref[...], 0.0), axis=1, keepdims=True)
        total = total + jnp.sum(jnp.where(flag_fresh, fresh_probs, 0.0), axis=1, keepdims=True)
        m_ref[...] = acc_ref[:, h * width : (h + 1) * width] / total
        for g in range(group):
            at = (h * group + g) * width
            out_ref[:, at : at + width] = m_ref[pl.ds(g, rows // group, stride=group), :].astype(bf16)
    for copy in weight_copies:
        copy.wait()


def attend_pool(index, queries, fresh_kv, kv_pool, page_table, context_lengths, gate_up, down_proj):
    step_count, req_count, head_count, head_width = queries.shape
    pool_pages, page_len, kv_heads, _ = kv_pool.shape
    group = head_count // kv_heads
    blocks = next(b for b in (4, 5, 2, 1) if pool_pages * page_len * 2 % (b * head_width) == 0)
    tokens = pool_pages * page_len
    rows, columns = step_count * req_count * group, tokens * 2 // blocks
    bf16, f32 = jnp.bfloat16, jnp.float32
    vmem, hbm = pl.BlockSpec(memory_space=pltpu.VMEM), pl.BlockSpec(memory_space=pltpu.HBM)
    own = step_count * req_count
    return pl.pallas_call(
        functools.partial(attend_kernel, req_count, group, page_len, blocks),
        out_shape=(
            jax.ShapeDtypeStruct((own, head_count * head_width), bf16),
            pltpu.VMEM(gate_up.shape, bf16),
            pltpu.VMEM(down_proj.shape, bf16),
        ),
        in_specs=[pl.BlockSpec(memory_space=pltpu.SMEM)] * 3 + [hbm] * 5,
        out_specs=(vmem, vmem, vmem),
        scratch_shapes=[
            pltpu.VMEM((own, head_count, head_width), bf16),
            pltpu.VMEM((tokens, 2, head_width), bf16),
            pltpu.VMEM((tokens, 2, head_width), bf16),
            pltpu.VMEM((own, 2, head_width), bf16),
            pltpu.VMEM((own, 2, head_width), bf16),
            pltpu.VMEM((blocks, rows, columns), f32),
            pltpu.VMEM((rows, 2 * head_width), f32),
            pltpu.VMEM((rows, head_width), f32),
            pltpu.VMEM((rows, head_width), f32),
            pltpu.SMEM((pool_pages,), jnp.int32),
            pltpu.SemaphoreType.DMA((blocks,)),
            pltpu.SemaphoreType.DMA((blocks,)),
            pltpu.SemaphoreType.DMA((3,)),
            pltpu.SemaphoreType.DMA((2,)),
        ],
        compiler_params=pltpu.CompilerParams(vmem_limit_bytes=24 * 1024 * 1024),
        name="attend_pool",
    )(
        index,
        page_table,
        context_lengths,
        *[
            pltpu.with_memory_space_constraint(value, pltpu.HBM)
            for value in (
                queries.reshape(own, head_count, head_width),
                fresh_kv.reshape(own, kv_heads, 2 * head_width),
                kv_pool.reshape(tokens, kv_heads, 2 * head_width),
                gate_up,
                down_proj,
            )
        ],
    )


def exchange(value, axis, mask):
    count = lax.axis_size(axis)
    return lax.ppermute(value, axis, [(i, i ^ mask) for i in range(count)])


def reorder(blocks, index, low=0):
    blocks = list(blocks)
    for bit in range(low, len(blocks).bit_length() - 1):
        flip = (index >> bit) & 1 == 1
        blocks = [jnp.where(flip, blocks[j ^ (1 << bit)], blocks[j]) for j in range(len(blocks))]
    return blocks


def split_pair(value):
    high = lax.reduce_precision(value, 8, 7)
    return high.astype(jnp.bfloat16), (value - high).astype(jnp.bfloat16)


def where_am_i(index_ref):
    return index_ref[0], index_ref[1]


def project_kernel(pieces, index_ref, *refs):
    weight_ref, keep_ref, send_ref = refs[2 * pieces :]
    dp_index, x_index = where_am_i(index_ref)
    rows = jnp.concatenate([ref[...] for ref in refs[: 2 * pieces]], axis=0)
    near = pieces // 2
    value = jnp.dot(rows, weight_ref[...], preferred_element_type=jnp.float32)
    own = rows.shape[0] // (2 * pieces)
    stay = (dp_index // 2) // near == x_index
    for at, ref in ((0, keep_ref), (pieces, send_ref)):
        blocks = [value[(at + k) * own : (at + k + 1) * own] for k in range(pieces)]
        for k in range(pieces):
            ref[k] = jnp.where(stay, blocks[k], blocks[k ^ near]).astype(jnp.bfloat16)


def pair_kernel(keep_ref, got_ref, *outs):
    block = keep_ref.shape[2]
    for k, out in enumerate(outs):
        out[:, :block] = keep_ref[k]
        out[:, block:] = got_ref[k]


def stream_kernel(pieces, experts, index_ref, *refs):
    f32, bf16 = jnp.float32, jnp.bfloat16
    gots = refs[:pieces]
    residual_ref, gain_ref, ids_ref, weight_ref, stream_ref, rows_ref = refs[pieces:]
    dp_index, _ = where_am_i(index_ref)
    near = pieces // 2
    width = stream_ref.shape[1]
    extra = rows_ref.shape[1] - width
    sums = [gots[k][...].astype(f32) + gots[k + near][...].astype(f32) for k in range(near)]
    sums = reorder(sums, (dp_index // 2) % near)
    block = sums[0].shape[1] // 2
    at = 0
    square = 0.0
    for both in sums:
        for part in reorder([both[:, :block], both[:, block:]], dp_index % 2):
            cut = slice(at, at + block)
            value = part + residual_ref[:, cut].astype(f32)
            stream_ref[:, cut] = value
            rows_ref[:, cut] = (value * gain_ref[:, cut]).astype(bf16)
            square = square + jnp.sum(value * value, axis=1, keepdims=True)
            at += block
    column = lax.broadcasted_iota(jnp.int32, (experts, extra), 1) - 2
    expert = lax.broadcasted_iota(jnp.int32, (experts, extra), 0)
    routes = []
    for step in range(ids_ref.shape[0]):
        ids, weights = ids_ref[step], weight_ref[step]
        share = weights / jnp.sum(weights, axis=0, keepdims=True)
        label = lax.broadcasted_iota(jnp.int32, (experts, ids.shape[1]), 0)
        table = jnp.zeros(label.shape, f32)
        for k in range(ids.shape[0]):
            table = table + jnp.where(label == ids[k : k + 1], share[k : k + 1], 0.0)
        high = table.astype(bf16)
        low = (table - high.astype(f32)).astype(bf16)
        spread = 0.0
        for value, shift in ((high, 0), (low, experts)):
            chosen = jnp.where(column == expert + shift, 1.0, 0.0).astype(bf16)
            spread = spread + lax.dot_general(
                value, chosen, (((0,), (0,)), ((), ())), preferred_element_type=f32
            )
        routes.append(spread)
    routes = jnp.concatenate(routes, axis=0)
    high = square.astype(bf16).astype(f32)
    lane = lax.broadcasted_iota(jnp.int32, routes.shape, 1)
    routes = jnp.where(lane == 0, high, jnp.where(lane == 1, square - high, routes))
    rows_ref[:, width:] = routes.astype(bf16)


def gate_up_kernel(pieces, index_ref, *refs):
    weight_ref, keep_ref, send_ref, own_ref = refs[pieces:]
    local_experts, _, width, hidden = weight_ref.shape
    part = hidden // 2
    first = index_ref[1] == 0
    rows = jnp.concatenate([ref[:, :width] for ref in refs[:pieces]], axis=0)
    for e in range(local_experts):
        for side in range(2):
            at = 2 * e + side
            value = jnp.dot(rows, weight_ref[e, side], preferred_element_type=jnp.float32)
            keep_ref[at] = jnp.where(first, value[:, :part], value[:, part:])
            send = jnp.where(first, value[:, part:], value[:, :part])
            send_ref[:, at * part : (at + 1) * part] = send.astype(jnp.bfloat16)
    extra = jnp.concatenate([ref[:, width:] for ref in refs[:pieces]], axis=0)
    own_ref[...] = extra
    send_ref[:, 2 * local_experts * part :] = extra


def act_kernel(local_experts, experts, width, index_ref, keep_ref, got_ref, own_ref, out_ref):
    f32 = jnp.float32
    part = keep_ref.shape[2]
    own = own_ref[...].astype(f32)
    lane = lax.broadcasted_iota(jnp.int32, own.shape, 1)
    other = got_ref[:, 2 * local_experts * part :].astype(f32)
    square = jnp.sum(jnp.where(lane < 2, own + other, 0.0), axis=1, keepdims=True)
    inverse = lax.rsqrt(square / width + EPS)
    for e in range(local_experts):
        column = 2 + index_ref[0] * local_experts + e
        chosen = (lane == column) | (lane == column + experts)
        share = jnp.sum(jnp.where(chosen, own, 0.0), axis=1, keepdims=True)
        gate = keep_ref[2 * e] + got_ref[:, 2 * e * part : (2 * e + 1) * part].astype(f32)
        up = keep_ref[2 * e + 1] + got_ref[:, (2 * e + 1) * part : (2 * e + 2) * part].astype(f32)
        gate = gate * inverse
        act = gate / (1.0 + jnp.exp(-gate)) * (up * inverse) * share
        out_ref[:, e * part : (e + 1) * part] = act.astype(jnp.bfloat16)


def down_kernel(index_ref, act_ref, got_ref, weight_ref, keep_ref, send_ref):
    local_experts, hidden, width = weight_ref.shape
    part = hidden // 2
    half = keep_ref.shape[0]
    first = index_ref[1] == 0
    acts = []
    for e in range(local_experts):
        own = act_ref[:, e * part : (e + 1) * part]
        got = got_ref[:, e * part : (e + 1) * part]
        acts += [jnp.where(first, own, got), jnp.where(first, got, own)]
    acts = jnp.concatenate(acts, axis=1)
    step = 512
    for at in range(0, width, step):
        value = jnp.zeros((acts.shape[0], step), jnp.float32)
        for e in range(local_experts):
            value = value + jnp.dot(
                acts[:, e * hidden : (e + 1) * hidden],
                weight_ref[e, :, at : at + step],
                preferred_element_type=jnp.float32,
            )
        keep_ref[:, at : at + step] = value[:half]
        send_ref[:, at : at + step] = value[half:].astype(jnp.bfloat16)


def hold_kernel(piece_ref, out_ref):
    out_ref[...] = piece_ref[...]


def fold_kernel(keep_ref, got_ref, *outs):
    own = outs[0].shape[0]
    for k, out in enumerate(outs):
        cut = slice(k * own, (k + 1) * own)
        value = keep_ref[cut] + got_ref[cut].astype(jnp.float32)
        out[...] = value.astype(out.dtype)


def small_call(kernel, outs, *args, index=None, flops=0, limit=8):
    vmem, smem = pl.BlockSpec(memory_space=pltpu.VMEM), pl.BlockSpec(memory_space=pltpu.SMEM)
    specs = [vmem] * len(args)
    if index is not None:
        specs, args = [smem] + specs, (index,) + args
    return pl.pallas_call(
        kernel,
        out_shape=tuple(jax.ShapeDtypeStruct(shape, dtype) for shape, dtype in outs),
        in_specs=specs,
        out_specs=(vmem,) * len(outs),
        compiler_params=pltpu.CompilerParams(vmem_limit_bytes=limit * 1024 * 1024),
        cost_estimate=pl.CostEstimate(flops=flops, bytes_accessed=0, transcendentals=0)
        if flops
        else None,
    )(*args)


def expert_chunk(rows, x_index, dp_index, gate_up, down_proj, expert_total):
    bf16, f32 = jnp.bfloat16, jnp.float32
    x_count = lax.axis_size("expert")
    local_experts, _, width, hidden = gate_up.shape
    part = hidden // x_count
    own = rows[:, width:]
    rows = rows[:, :width]
    routes = own[:, 2 : 2 + 2 * expert_total].astype(f32)
    routes = routes[:, :expert_total] + routes[:, expert_total:]
    share = lax.dynamic_slice_in_dim(routes, dp_index * local_experts, local_experts, axis=1)
    products = [
        jnp.dot(rows, gate_up[e, s], preferred_element_type=f32)
        for e in range(local_experts)
        for s in range(2)
    ]
    parts = [
        reorder([p[:, k * part : (k + 1) * part] for k in range(x_count)], x_index) for p in products
    ]
    sums = [p[0] for p in parts]
    square = jnp.sum(own[:, :2].astype(f32), axis=1)
    for k in range(1, x_count):
        sent = jnp.concatenate([p[k].astype(bf16) for p in parts] + [own[:, :2]], axis=1)
        got = exchange(sent, "expert", k).astype(f32)
        sums = [s + got[:, i * part : (i + 1) * part] for i, s in enumerate(sums)]
        square = square + jnp.sum(got[:, len(sums) * part :], axis=1)
    inverse = lax.rsqrt(square / (width * x_count) + EPS)[:, None]
    total = 0.0
    for e in range(local_experts):
        gate, up = sums[2 * e] * inverse, sums[2 * e + 1] * inverse
        act = (jax.nn.silu(gate) * up * share[:, e : e + 1]).astype(bf16)
        pieces = [act] + [exchange(act, "expert", k) for k in range(1, x_count)]
        act = jnp.concatenate(reorder(pieces, x_index), axis=1)
        total = total + jnp.dot(act, down_proj[e], preferred_element_type=f32)
    half = total.shape[0] // 2
    return total[:half], total[half:].astype(bf16)


def body_plain(
    queries,
    fresh_kv,
    kv_pool,
    page_table,
    context_lengths,
    residual,
    out_weight,
    norm_gain,
    expert_ids,
    route_weights,
    gate_up,
    down_proj,
):
    bf16, f32 = jnp.bfloat16, jnp.float32
    dp_count, x_count = lax.axis_size("dp"), lax.axis_size("expert")
    dp_index, x_index = lax.axis_index("dp"), lax.axis_index("expert")
    chips = dp_count // 2
    chip_index, core_index = dp_index // 2, dp_index % 2
    local_experts, _, width, _ = gate_up.shape
    expert_total = local_experts * dp_count
    steps, reqs = queries.shape[:2]
    own = steps * reqs

    attended = attend(queries, fresh_kv, kv_pool, page_table, context_lengths)
    attended = attended.reshape(own, attended.shape[2])
    mine = jnp.stack([attended] + [exchange(attended, "dp", 2 * k) for k in range(1, chips)])
    gathered = jnp.stack([mine, exchange(mine, "dp", 1)])
    gathered = gathered.reshape(dp_count * own, attended.shape[1])

    columns = jnp.dot(gathered, out_weight, preferred_element_type=f32).astype(bf16)
    block = columns.shape[1]
    columns = columns.reshape(2, chips, own, block)
    swapped = exchange(columns[1], "dp", 1)
    paired = [jnp.concatenate([columns[0, k], swapped[k]], axis=1) for k in range(chips)]
    near = chips // x_count
    low = near.bit_length() - 1
    paired = reorder(paired, ((chip_index // near) ^ x_index) * near, low)
    parts = [0.0] * near
    for k in range(chips):
        moves = []
        for z in range(chips):
            for c in range(2):
                for x in range(x_count):
                    away = (z // near) ^ x
                    there = z ^ k ^ (away * near)
                    moves.append(((2 * z + c) * x_count + x, (2 * there + c) * x_count + z // near))
        got = lax.ppermute(paired[k], ("dp", "expert"), moves).astype(f32)
        parts[k % near] = parts[k % near] + got
    parts = [
        reorder([p[:, c * block : (c + 1) * block] for c in range(2)], core_index)
        for p in reorder(parts, chip_index % near)
    ]
    stream = jnp.concatenate([b for pair in parts for b in pair], axis=1)
    stream = stream + residual.astype(f32).reshape(own, width)

    share = route_weights / jnp.sum(route_weights, axis=2, keepdims=True)
    catalog = jnp.arange(expert_total, dtype=jnp.int32)
    named = expert_ids[..., None] == catalog
    routed = jnp.sum(jnp.where(named, share[..., None], 0.0), axis=2)
    routed_high, routed_low = split_pair(routed.reshape(own, expert_total))
    square_high, square_low = split_pair(jnp.sum(stream * stream, axis=1, keepdims=True))
    extra = -(-(2 * expert_total + 2) // 128) * 128
    rows = jnp.concatenate(
        [
            (stream * norm_gain[None, :]).astype(bf16),
            square_high,
            square_low,
            routed_high,
            routed_low,
            jnp.zeros((own, extra - 2 * expert_total - 2), bf16),
        ],
        axis=1,
    )
    from_chip = [rows] + [exchange(rows, "dp", 2 * k) for k in range(1, chips)]
    result = stream
    for chunk in (range(chips // 2, chips), range(chips // 2)):
        mine = jnp.concatenate([from_chip[k] for k in chunk], axis=0)
        taken = jnp.concatenate([mine, exchange(mine, "dp", 1)], axis=0)
        keep, send = expert_chunk(taken, x_index, dp_index, gate_up, down_proj, expert_total)
        keep = keep + exchange(send, "dp", 1).astype(f32)
        for i, k in enumerate(chunk):
            piece = keep[i * own : (i + 1) * own]
            if k > 0:
                piece = exchange(piece.astype(bf16), "dp", 2 * k).astype(f32)
            result = result + piece
    return result.reshape(steps, reqs, width).astype(bf16)


def body_fast(
    queries,
    fresh_kv,
    kv_pool,
    page_table,
    context_lengths,
    residual,
    out_weight,
    norm_gain,
    expert_ids,
    route_weights,
    gate_up,
    down_proj,
):
    bf16, f32 = jnp.bfloat16, jnp.float32
    dp_count, x_count = lax.axis_size("dp"), lax.axis_size("expert")
    dp_index, x_index = lax.axis_index("dp"), lax.axis_index("expert")
    index = jnp.stack([dp_index, x_index]).astype(jnp.int32)
    chips = dp_count // 2
    local_experts, _, width, hidden = gate_up.shape
    part = hidden // 2
    expert_total = local_experts * dp_count
    steps, reqs = queries.shape[:2]
    own = steps * reqs

    attended, gate_up, down_proj = attend_pool(
        index, queries, fresh_kv, kv_pool, page_table, context_lengths, gate_up, down_proj
    )
    head_cols = attended.shape[1]
    mine = [attended] + [exchange(attended, "dp", 2 * k) for k in range(1, chips)]
    mine = mine + [exchange(piece, "dp", 1) for piece in mine]
    block = out_weight.shape[1]
    keep, send = small_call(
        functools.partial(project_kernel, chips),
        [((chips, own, block), bf16)] * 2,
        *mine,
        out_weight,
        index=index,
        flops=2 * dp_count * own * head_cols * block,
    )
    paired = small_call(
        pair_kernel, [((own, 2 * block), bf16)] * chips, keep, exchange(send, "dp", 1)
    )
    near = chips // x_count
    arrived = []
    for k in range(chips):
        moves = []
        for z in range(chips):
            for c in range(2):
                for x in range(x_count):
                    away = (z // near) ^ x
                    there = z ^ k ^ (away * near)
                    moves.append(((2 * z + c) * x_count + x, (2 * there + c) * x_count + z // near))
        arrived.append(lax.ppermute(paired[k], ("dp", "expert"), moves))

    extra = -(-(2 * expert_total + 2) // 128) * 128
    stream, rows = small_call(
        functools.partial(stream_kernel, chips, expert_total),
        [((own, width), f32), ((own, width + extra), bf16)],
        *arrived,
        residual.reshape(own, width),
        norm_gain.reshape(1, width),
        jnp.swapaxes(expert_ids, 1, 2),
        jnp.swapaxes(route_weights, 1, 2),
        index=index,
    )
    from_chip = [rows]
    for k in range(1, chips):
        from_chip.append(exchange(rows, "dp", 2 * k))
        if k == 1 or k % 2 == 0:
            (from_chip[k],) = small_call(hold_kernel, [(rows.shape, bf16)], from_chip[k])
    result = stream
    for chunk in (range(1, chips, 2), range(0, chips, 2)):
        pieces = [from_chip[k] for k in chunk]
        pieces = pieces + [exchange(piece, "dp", 1) for piece in pieces]
        count = len(pieces) * own
        keep, send, extras = small_call(
            functools.partial(gate_up_kernel, len(pieces)),
            [
                ((2 * local_experts, count, part), f32),
                ((count, 2 * local_experts * part + extra), bf16),
                ((count, extra), bf16),
            ],
            *pieces,
            gate_up,
            index=index,
            flops=4 * count * width * hidden * local_experts,
        )
        got = exchange(send, "expert", 1)
        (act,) = small_call(
            functools.partial(act_kernel, local_experts, expert_total, x_count * width),
            [((count, local_experts * part), bf16)],
            keep,
            got,
            extras,
            index=index,
        )
        got = exchange(act, "expert", 1)
        keep, send = small_call(
            down_kernel,
            [((count // 2, width), f32), ((count // 2, width), bf16)],
            act,
            got,
            down_proj,
            index=index,
            flops=2 * count * width * hidden * local_experts,
        )
        folded = small_call(
            fold_kernel,
            [((own, width), bf16 if k else f32) for k in chunk],
            keep,
            exchange(send, "dp", 1),
        )
        for k, piece in zip(chunk, folded):
            if k > 0:
                piece = exchange(piece, "dp", 2 * k).astype(f32)
            result = result + piece
    return result.reshape(steps, reqs, width).astype(bf16)


def body(*args):
    fast = (
        args[2].shape[2] == 2
        and lax.axis_size("expert") == 2
        and lax.axis_size("dp") >= 4
        and args[10].shape[3] % 256 == 0
        and args[10].shape[2] % 512 == 0
    )
    if not fast:
        return body_plain(*args)
    return body_fast(*args)


def solution(mesh):
    return jax.shard_map(
        body,
        mesh=mesh,
        in_specs=(
            P(None, ("groups", "dp"), "expert", None),
            P(None, ("groups", "dp"), "expert", None),
            P(("groups", "dp"), None, "expert", None),
            P(("groups", "dp"), None),
            P(("groups", "dp")),
            P(None, ("groups", "dp"), "expert"),
            P("expert", "dp"),
            P("expert"),
            P(None, ("groups", "dp"), None),
            P(None, ("groups", "dp"), None),
            P("dp", None, "expert", None),
            P("dp", None, "expert"),
        ),
        out_specs=P(None, ("groups", "dp"), "expert"),
        check_vma=False,
    )
```

```python
import functools
import math

import jax
import jax.numpy as jnp
from jax import lax
from jax.experimental import pallas as pl
from jax.experimental.pallas import tpu as pltpu

from jax.sharding import PartitionSpec as P

NEG = -1e30
EPS = 1e-06
EXACT = lax.Precision.HIGHEST


def page_owners(table, lengths, pool_pages, page_len):
    pages = jnp.arange(pool_pages, dtype=jnp.int32)
    matches = table[:, :, None] == pages[None, None, :]
    ownership = jnp.any(matches, axis=1)
    slot_index = jnp.arange(table.shape[1], dtype=jnp.int32)
    position = jnp.sum(jnp.where(matches, slot_index[None, :, None], 0), axis=(0, 1))
    owner_length = jnp.sum(jnp.where(ownership, lengths[:, None], 0), axis=0)
    live_count = jnp.clip(owner_length - position * page_len, 0, page_len)
    return (ownership, live_count)


def attend(query_block, fresh_block, pool_block, table_block, length_block):
    step_count, req_count, head_count, head_width = query_block.shape
    pool_pages, page_len, kv_heads, _ = pool_block.shape
    group_size = head_count // kv_heads
    score_scale = 1.0 / math.sqrt(head_width)
    ownership, live_count = page_owners(table_block, length_block, pool_pages, page_len)
    owned_f = ownership.astype(jnp.float32)
    grouped = query_block.reshape(step_count, req_count, kv_heads, group_size, head_width)
    page_query = jnp.einsum(
        "rp,srkgd->pskgd",
        ownership.astype(jnp.bfloat16),
        grouped,
        preferred_element_type=jnp.float32,
    ).astype(jnp.bfloat16)
    key_rows = pool_block[..., :head_width]
    value_rows = pool_block[..., head_width:]
    page_scores = (
        jnp.einsum("pskgd,ptkd->pskgt", page_query, key_rows, preferred_element_type=jnp.float32)
        * score_scale
    )
    in_page = jnp.arange(page_len)[None, :] < live_count[:, None]
    page_scores = jnp.where(in_page[:, None, None, None, :], page_scores, NEG)
    fresh_keys = fresh_block[..., :head_width]
    fresh_values = fresh_block[..., head_width:]
    fresh_scores = (
        jnp.einsum("srkgd,urkd->srkgu", grouped, fresh_keys, preferred_element_type=jnp.float32)
        * score_scale
    )
    causal = jnp.arange(step_count)[:, None] >= jnp.arange(step_count)[None, :]
    fresh_scores = jnp.where(causal[:, None, None, None, :], fresh_scores, NEG)
    page_best = jnp.max(page_scores, axis=4)
    row_best = jnp.max(jnp.where(ownership[:, :, None, None, None], page_best[None], NEG), axis=1)
    row_best = jnp.maximum(row_best, jnp.moveaxis(jnp.max(fresh_scores, axis=4), 0, 1))
    owner_best = jnp.einsum("rp,rskg->pskg", owned_f, row_best, precision=EXACT)
    page_probs = jnp.exp(page_scores - owner_best[..., None])
    page_sum = jnp.sum(page_probs, axis=4)
    page_acc = jnp.einsum(
        "pskgt,ptkd->pskgd",
        page_probs.astype(jnp.bfloat16),
        value_rows,
        preferred_element_type=jnp.float32,
    )
    denominator = jnp.einsum("rp,pskg->rskg", owned_f, page_sum, precision=EXACT)
    numerator = jnp.einsum("rp,pskgd->rskgd", owned_f, page_acc, precision=EXACT)
    fresh_probs = jnp.exp(fresh_scores - jnp.moveaxis(row_best, 1, 0)[..., None])
    denominator = denominator + jnp.moveaxis(jnp.sum(fresh_probs, axis=4), 0, 1)
    numerator = numerator + jnp.einsum(
        "srkgu,urkd->rskgd",
        fresh_probs.astype(jnp.bfloat16),
        fresh_values,
        preferred_element_type=jnp.float32,
    )
    attended = jnp.moveaxis(numerator / denominator[..., None], 1, 0)
    return attended.reshape(step_count, req_count, head_count * head_width).astype(jnp.bfloat16)


def attend_kernel(
    req_count, group, page_len, blocks, index_ref, table_hbm, q_hbm, fresh_hbm, kv_hbm, gate_up_hbm, down_hbm,
    out_ref, gate_up_ref, down_ref, q_ref, kbuf, vbuf, fkbuf, fvbuf, s_ref, acc_ref, l_ref, m_ref, code_ref, table_ref, ksem, vsem, fsem, wsem,
):
    f32, bf16 = jnp.float32, jnp.bfloat16
    width = q_ref.shape[2]
    tokens = kbuf.shape[0] // blocks
    columns = 2 * tokens
    pages = tokens // page_len
    rows = q_ref.shape[0] * group

    def fetch(half, buf, sem, b):
        part = pl.ds(b * tokens, tokens)
        return pltpu.make_async_copy(
            kv_hbm.at[part, :, pl.ds(half * width, width)], buf.at[part], sem.at[b]
        )

    fresh_copies = [
        pltpu.make_async_copy(fresh_hbm.at[:, :, pl.ds(h * width, width)], buf, fsem.at[h])
        for h, buf in enumerate((fkbuf, fvbuf))
    ]
    fresh_copies.append(pltpu.make_async_copy(q_hbm, q_ref, fsem.at[2]))
    table_copy = pltpu.make_async_copy(table_hbm, table_ref, fsem.at[3])
    table_copy.start()
    for copy in fresh_copies:
        copy.start()
    lax.fori_loop(0, blocks, lambda b, c: (fetch(0, kbuf, ksem, b).start(), c)[1], 0)
    lax.fori_loop(0, blocks, lambda b, c: (fetch(1, vbuf, vsem, b).start(), c)[1], 0)
    weight_copies = [
        pltpu.make_async_copy(gate_up_hbm, gate_up_ref, wsem.at[0]),
        pltpu.make_async_copy(down_hbm, down_ref, wsem.at[1]),
    ]
    for copy in weight_copies:
        copy.start()

    def clear(p, c):
        code_ref[p] = 0
        return c

    lax.fori_loop(0, blocks * pages, clear, 0, unroll=16)
    table_copy.wait()
    for r in range(req_count):
        length = index_ref[2 + r]

        def put(j, c, r=r, length=length):
            code_ref[table_ref[r, j]] = r * 32 + jnp.minimum(length - j * page_len, page_len)
            return c

        count = (length + page_len - 1) // page_len

        def four(i, c, r=r, length=length):
            spots = [table_ref[r, 4 * i + k] for k in range(4)]
            for k, spot in enumerate(spots):
                code_ref[spot] = r * 32 + jnp.minimum(length - (4 * i + k) * page_len, page_len)
            return c

        lax.fori_loop(0, count // 4, four, 0)
        lax.fori_loop(count // 4 * 4, count, put, 0)
    lane_page = lax.broadcasted_iota(jnp.int32, (1, width), 1) // (2 * page_len)
    per_tile = width // (2 * page_len)

    def codes(b):
        tiles = []
        for t in range(columns // width):
            at = b * pages + t * per_tile
            tile = jnp.zeros((1, width), jnp.int32)
            for i in range(per_tile):
                tile = jnp.where(lane_page == i, code_ref[at + i], tile)
            tiles.append(tile)
        return jnp.concatenate(tiles, axis=1)

    for copy in fresh_copies:
        copy.wait()

    q = q_ref[...].astype(f32)
    q2 = jnp.concatenate(
        [q[:, :group].reshape(rows, width), q[:, group:].reshape(rows, width)], axis=1
    ).astype(bf16)
    row = lax.broadcasted_iota(jnp.int32, (rows, 1), 0) // group
    row_req, row_step = row % req_count, row // req_count

    def widen(x):
        even = lax.broadcasted_iota(jnp.int32, x.shape, 0) % 2 == 0
        x = x.astype(f32)
        return jnp.concatenate(
            [jnp.where(even, x, 0.0), jnp.where(even, 0.0, x)], axis=1
        ).astype(bf16)

    def scores(keys):
        flat = keys.T.astype(f32)
        even = lax.broadcasted_iota(jnp.int32, (1, keys.shape[0]), 1) % 2 == 0
        both = jnp.concatenate([jnp.where(even, flat, 0.0), jnp.where(even, 0.0, flat)], axis=0)
        return jnp.dot(q2, both.astype(bf16), preferred_element_type=f32)

    fresh = fkbuf.shape[0] * 2
    fresh_keys = fkbuf.reshape(fresh, width)[...]
    col = lax.broadcasted_iota(jnp.int32, (1, fresh), 1) // 2
    allowed = (col % req_count == row_req) & (col // req_count <= row_step)
    fresh_scores = jnp.where(allowed, scores(fresh_keys), NEG)

    m_ref[...] = jnp.full(m_ref.shape, NEG, f32)
    slot = lax.broadcasted_iota(jnp.int32, (1, columns), 1) // 2 % page_len

    def first(b, c):
        fetch(0, kbuf, ksem, b).wait()
        keys = kbuf.reshape(kbuf.shape[0] * 2, width)[pl.ds(b * columns, columns), :]
        code = codes(b)
        owner = jnp.where(slot < (code & 31), code >> 5, -1)
        s = jnp.where(owner == row_req, scores(keys), NEG)
        s_ref[b] = s
        m = m_ref[...]
        for t in range(columns // width):
            m = jnp.maximum(m, s[:, t * width : (t + 1) * width])
        m_ref[...] = m
        return c

    lax.fori_loop(0, blocks, first, 0)

    even = lax.broadcasted_iota(jnp.int32, (1, width), 1) % 2 == 0
    even_fresh = lax.broadcasted_iota(jnp.int32, (1, fresh), 1) % 2 == 0

    def best(flag, flag_fresh):
        pool = jnp.max(jnp.where(flag, m_ref[...], NEG), axis=1, keepdims=True)
        new = jnp.max(jnp.where(flag_fresh, fresh_scores, NEG), axis=1, keepdims=True)
        return jnp.maximum(pool, new)

    best_even, best_odd = best(even, even_fresh), best(~even, ~even_fresh)
    m_ref[...] = jnp.where(even, best_even, best_odd)
    rate = math.log2(math.e) / math.sqrt(width)
    fresh_probs = jnp.exp2((fresh_scores - jnp.where(even_fresh, best_even, best_odd)) * rate)
    acc_ref[...] = jnp.dot(
        fresh_probs.astype(bf16), widen(fvbuf.reshape(fresh, width)[...]), preferred_element_type=f32
    )
    l_ref[...] = jnp.zeros(l_ref.shape, f32)

    def second(b, c):
        fetch(1, vbuf, vsem, b).wait()
        values = vbuf.reshape(vbuf.shape[0] * 2, width)[pl.ds(b * columns, columns), :]
        m = m_ref[...]
        total = l_ref[...]
        probs = []
        for t in range(columns // width):
            p = jnp.exp2((s_ref[b, :, t * width : (t + 1) * width] - m) * rate)
            total = total + p
            probs.append(p.astype(bf16))
        l_ref[...] = total
        acc_ref[...] += jnp.dot(
            jnp.concatenate(probs, axis=1), widen(values), preferred_element_type=f32
        )
        return c

    lax.fori_loop(0, blocks, second, 0)

    for h, (flag, flag_fresh) in enumerate(((even, even_fresh), (~even, ~even_fresh))):
        total = jnp.sum(jnp.where(flag, l_ref[...], 0.0), axis=1, keepdims=True)
        total = total + jnp.sum(jnp.where(flag_fresh, fresh_probs, 0.0), axis=1, keepdims=True)
        m_ref[...] = acc_ref[:, h * width : (h + 1) * width] / total
        for g in range(group):
            at = (h * group + g) * width
            out_ref[:, at : at + width] = m_ref[pl.ds(g, rows // group, stride=group), :].astype(bf16)
    for copy in weight_copies:
        copy.wait()


def attend_pool(index, queries, fresh_kv, kv_pool, page_table, gate_up, down_proj):
    step_count, req_count, head_count, head_width = queries.shape
    pool_pages, page_len, kv_heads, _ = kv_pool.shape
    group = head_count // kv_heads
    blocks = next(b for b in (4, 5, 2, 1) if pool_pages * page_len * 2 % (b * head_width) == 0)
    tokens = pool_pages * page_len
    rows, columns = step_count * req_count * group, tokens * 2 // blocks
    bf16, f32 = jnp.bfloat16, jnp.float32
    vmem, hbm = pl.BlockSpec(memory_space=pltpu.VMEM), pl.BlockSpec(memory_space=pltpu.HBM)
    own = step_count * req_count
    return pl.pallas_call(
        functools.partial(attend_kernel, req_count, group, page_len, blocks),
        out_shape=(
            jax.ShapeDtypeStruct((own, head_count * head_width), bf16),
            pltpu.VMEM(gate_up.shape, bf16),
            pltpu.VMEM(down_proj.shape, bf16),
        ),
        in_specs=[pl.BlockSpec(memory_space=pltpu.SMEM)] + [hbm] * 6,
        out_specs=(vmem, vmem, vmem),
        scratch_shapes=[
            pltpu.VMEM((own, head_count, head_width), bf16),
            pltpu.VMEM((tokens, 2, head_width), bf16),
            pltpu.VMEM((tokens, 2, head_width), bf16),
            pltpu.VMEM((own, 2, head_width), bf16),
            pltpu.VMEM((own, 2, head_width), bf16),
            pltpu.VMEM((blocks, rows, columns), f32),
            pltpu.VMEM((rows, 2 * head_width), f32),
            pltpu.VMEM((rows, head_width), f32),
            pltpu.VMEM((rows, head_width), f32),
            pltpu.SMEM((pool_pages,), jnp.int32),
            pltpu.SMEM(page_table.shape, jnp.int32),
            pltpu.SemaphoreType.DMA((blocks,)),
            pltpu.SemaphoreType.DMA((blocks,)),
            pltpu.SemaphoreType.DMA((4,)),
            pltpu.SemaphoreType.DMA((2,)),
        ],
        compiler_params=pltpu.CompilerParams(vmem_limit_bytes=24 * 1024 * 1024),
        name="attend_pool",
    )(
        index,
        *[
            pltpu.with_memory_space_constraint(value, pltpu.HBM)
            for value in (
                page_table,
                queries.reshape(own, head_count, head_width),
                fresh_kv.reshape(own, kv_heads, 2 * head_width),
                kv_pool.reshape(tokens, kv_heads, 2 * head_width),
                gate_up,
                down_proj,
            )
        ],
    )


def exchange(value, axis, mask):
    count = lax.axis_size(axis)
    return lax.ppermute(value, axis, [(i, i ^ mask) for i in range(count)])


def reorder(blocks, index, low=0):
    blocks = list(blocks)
    for bit in range(low, len(blocks).bit_length() - 1):
        flip = (index >> bit) & 1 == 1
        blocks = [jnp.where(flip, blocks[j ^ (1 << bit)], blocks[j]) for j in range(len(blocks))]
    return blocks


def split_pair(value):
    high = lax.reduce_precision(value, 8, 7)
    return high.astype(jnp.bfloat16), (value - high).astype(jnp.bfloat16)


def where_am_i(index_ref):
    return index_ref[0], index_ref[1]


def project_kernel(pieces, index_ref, *refs):
    weight_ref, keep_ref, send_ref = refs[2 * pieces :]
    dp_index, x_index = where_am_i(index_ref)
    rows = jnp.concatenate([ref[...] for ref in refs[: 2 * pieces]], axis=0)
    near = pieces // 2
    value = jnp.dot(rows, weight_ref[...], preferred_element_type=jnp.float32)
    own = rows.shape[0] // (2 * pieces)
    stay = (dp_index // 2) // near == x_index
    for at, ref in ((0, keep_ref), (pieces, send_ref)):
        blocks = [value[(at + k) * own : (at + k + 1) * own] for k in range(pieces)]
        for k in range(pieces):
            ref[k] = jnp.where(stay, blocks[k], blocks[k ^ near]).astype(jnp.bfloat16)


def pair_kernel(keep_ref, got_ref, *outs):
    block = keep_ref.shape[2]
    for k, out in enumerate(outs):
        out[:, :block] = keep_ref[k]
        out[:, block:] = got_ref[k]


def stream_kernel(pieces, experts, index_ref, *refs):
    f32, bf16 = jnp.float32, jnp.bfloat16
    gots = refs[:pieces]
    residual_ref, gain_ref, ids_ref, weight_ref, stream_ref, rows_ref = refs[pieces:]
    dp_index, _ = where_am_i(index_ref)
    near = pieces // 2
    width = stream_ref.shape[1]
    extra = rows_ref.shape[1] - width
    sums = [gots[k][...].astype(f32) + gots[k + near][...].astype(f32) for k in range(near)]
    sums = reorder(sums, (dp_index // 2) % near)
    block = sums[0].shape[1] // 2
    at = 0
    square = 0.0
    for both in sums:
        for part in reorder([both[:, :block], both[:, block:]], dp_index % 2):
            cut = slice(at, at + block)
            value = part + residual_ref[:, cut].astype(f32)
            stream_ref[:, cut] = value
            rows_ref[:, cut] = (value * gain_ref[:, cut]).astype(bf16)
            square = square + jnp.sum(value * value, axis=1, keepdims=True)
            at += block
    column = lax.broadcasted_iota(jnp.int32, (experts, extra), 1) - 2
    expert = lax.broadcasted_iota(jnp.int32, (experts, extra), 0)
    routes = []
    for step in range(ids_ref.shape[0]):
        ids, weights = ids_ref[step], weight_ref[step]
        share = weights / jnp.sum(weights, axis=0, keepdims=True)
        label = lax.broadcasted_iota(jnp.int32, (experts, ids.shape[1]), 0)
        table = jnp.zeros(label.shape, f32)
        for k in range(ids.shape[0]):
            table = table + jnp.where(label == ids[k : k + 1], share[k : k + 1], 0.0)
        high = table.astype(bf16)
        low = (table - high.astype(f32)).astype(bf16)
        spread = 0.0
        for value, shift in ((high, 0), (low, experts)):
            chosen = jnp.where(column == expert + shift, 1.0, 0.0).astype(bf16)
            spread = spread + lax.dot_general(
                value, chosen, (((0,), (0,)), ((), ())), preferred_element_type=f32
            )
        routes.append(spread)
    routes = jnp.concatenate(routes, axis=0)
    high = square.astype(bf16).astype(f32)
    lane = lax.broadcasted_iota(jnp.int32, routes.shape, 1)
    routes = jnp.where(lane == 0, high, jnp.where(lane == 1, square - high, routes))
    rows_ref[:, width:] = routes.astype(bf16)


def gate_up_kernel(pieces, index_ref, *refs):
    weight_ref, keep_ref, send_ref, own_ref = refs[pieces:]
    local_experts, _, width, hidden = weight_ref.shape
    part = hidden // 2
    first = index_ref[1] == 0
    rows = jnp.concatenate([ref[:, :width] for ref in refs[:pieces]], axis=0)
    for e in range(local_experts):
        for side in range(2):
            at = 2 * e + side
            value = jnp.dot(rows, weight_ref[e, side], preferred_element_type=jnp.float32)
            keep_ref[at] = jnp.where(first, value[:, :part], value[:, part:])
            send = jnp.where(first, value[:, part:], value[:, :part])
            send_ref[:, at * part : (at + 1) * part] = send.astype(jnp.bfloat16)
    extra = jnp.concatenate([ref[:, width:] for ref in refs[:pieces]], axis=0)
    own_ref[...] = extra
    send_ref[:, 2 * local_experts * part :] = extra


def act_kernel(local_experts, experts, width, index_ref, keep_ref, got_ref, own_ref, out_ref):
    f32 = jnp.float32
    part = keep_ref.shape[2]
    own = own_ref[...].astype(f32)
    lane = lax.broadcasted_iota(jnp.int32, own.shape, 1)
    other = got_ref[:, 2 * local_experts * part :].astype(f32)
    square = jnp.sum(jnp.where(lane < 2, own + other, 0.0), axis=1, keepdims=True)
    inverse = lax.rsqrt(square / width + EPS)
    for e in range(local_experts):
        column = 2 + index_ref[0] * local_experts + e
        chosen = (lane == column) | (lane == column + experts)
        share = jnp.sum(jnp.where(chosen, own, 0.0), axis=1, keepdims=True)
        gate = keep_ref[2 * e] + got_ref[:, 2 * e * part : (2 * e + 1) * part].astype(f32)
        up = keep_ref[2 * e + 1] + got_ref[:, (2 * e + 1) * part : (2 * e + 2) * part].astype(f32)
        gate = gate * inverse
        act = gate / (1.0 + jnp.exp(-gate)) * (up * inverse) * share
        out_ref[:, e * part : (e + 1) * part] = act.astype(jnp.bfloat16)


def down_kernel(index_ref, act_ref, got_ref, weight_ref, keep_ref, send_ref):
    local_experts, hidden, width = weight_ref.shape
    part = hidden // 2
    half = keep_ref.shape[0]
    first = index_ref[1] == 0
    acts = []
    for e in range(local_experts):
        own = act_ref[:, e * part : (e + 1) * part]
        got = got_ref[:, e * part : (e + 1) * part]
        acts += [jnp.where(first, own, got), jnp.where(first, got, own)]
    acts = jnp.concatenate(acts, axis=1)
    step = 512
    for at in range(0, width, step):
        value = jnp.zeros((acts.shape[0], step), jnp.float32)
        for e in range(local_experts):
            value = value + jnp.dot(
                acts[:, e * hidden : (e + 1) * hidden],
                weight_ref[e, :, at : at + step],
                preferred_element_type=jnp.float32,
            )
        keep_ref[:, at : at + step] = value[:half]
        send_ref[:, at : at + step] = value[half:].astype(jnp.bfloat16)


def hold_kernel(piece_ref, out_ref):
    out_ref[...] = piece_ref[...]


def fold_kernel(keep_ref, got_ref, *outs):
    own = outs[0].shape[0]
    for k, out in enumerate(outs):
        cut = slice(k * own, (k + 1) * own)
        value = keep_ref[cut] + got_ref[cut].astype(jnp.float32)
        out[...] = value.astype(out.dtype)


def small_call(kernel, outs, *args, index=None, flops=0, limit=8):
    vmem, smem = pl.BlockSpec(memory_space=pltpu.VMEM), pl.BlockSpec(memory_space=pltpu.SMEM)
    specs = [vmem] * len(args)
    if index is not None:
        specs, args = [smem] + specs, (index,) + args
    return pl.pallas_call(
        kernel,
        out_shape=tuple(jax.ShapeDtypeStruct(shape, dtype) for shape, dtype in outs),
        in_specs=specs,
        out_specs=(vmem,) * len(outs),
        compiler_params=pltpu.CompilerParams(vmem_limit_bytes=limit * 1024 * 1024),
        cost_estimate=pl.CostEstimate(flops=flops, bytes_accessed=0, transcendentals=0)
        if flops
        else None,
    )(*args)


def expert_chunk(rows, x_index, dp_index, gate_up, down_proj, expert_total):
    bf16, f32 = jnp.bfloat16, jnp.float32
    x_count = lax.axis_size("expert")
    local_experts, _, width, hidden = gate_up.shape
    part = hidden // x_count
    own = rows[:, width:]
    rows = rows[:, :width]
    routes = own[:, 2 : 2 + 2 * expert_total].astype(f32)
    routes = routes[:, :expert_total] + routes[:, expert_total:]
    share = lax.dynamic_slice_in_dim(routes, dp_index * local_experts, local_experts, axis=1)
    products = [
        jnp.dot(rows, gate_up[e, s], preferred_element_type=f32)
        for e in range(local_experts)
        for s in range(2)
    ]
    parts = [
        reorder([p[:, k * part : (k + 1) * part] for k in range(x_count)], x_index) for p in products
    ]
    sums = [p[0] for p in parts]
    square = jnp.sum(own[:, :2].astype(f32), axis=1)
    for k in range(1, x_count):
        sent = jnp.concatenate([p[k].astype(bf16) for p in parts] + [own[:, :2]], axis=1)
        got = exchange(sent, "expert", k).astype(f32)
        sums = [s + got[:, i * part : (i + 1) * part] for i, s in enumerate(sums)]
        square = square + jnp.sum(got[:, len(sums) * part :], axis=1)
    inverse = lax.rsqrt(square / (width * x_count) + EPS)[:, None]
    total = 0.0
    for e in range(local_experts):
        gate, up = sums[2 * e] * inverse, sums[2 * e + 1] * inverse
        act = (jax.nn.silu(gate) * up * share[:, e : e + 1]).astype(bf16)
        pieces = [act] + [exchange(act, "expert", k) for k in range(1, x_count)]
        act = jnp.concatenate(reorder(pieces, x_index), axis=1)
        total = total + jnp.dot(act, down_proj[e], preferred_element_type=f32)
    half = total.shape[0] // 2
    return total[:half], total[half:].astype(bf16)


def body_plain(
    queries,
    fresh_kv,
    kv_pool,
    page_table,
    context_lengths,
    residual,
    out_weight,
    norm_gain,
    expert_ids,
    route_weights,
    gate_up,
    down_proj,
):
    bf16, f32 = jnp.bfloat16, jnp.float32
    dp_count, x_count = lax.axis_size("dp"), lax.axis_size("expert")
    dp_index, x_index = lax.axis_index("dp"), lax.axis_index("expert")
    chips = dp_count // 2
    chip_index, core_index = dp_index // 2, dp_index % 2
    local_experts, _, width, _ = gate_up.shape
    expert_total = local_experts * dp_count
    steps, reqs = queries.shape[:2]
    own = steps * reqs

    attended = attend(queries, fresh_kv, kv_pool, page_table, context_lengths)
    attended = attended.reshape(own, attended.shape[2])
    mine = jnp.stack([attended] + [exchange(attended, "dp", 2 * k) for k in range(1, chips)])
    gathered = jnp.stack([mine, exchange(mine, "dp", 1)])
    gathered = gathered.reshape(dp_count * own, attended.shape[1])

    columns = jnp.dot(gathered, out_weight, preferred_element_type=f32).astype(bf16)
    block = columns.shape[1]
    columns = columns.reshape(2, chips, own, block)
    swapped = exchange(columns[1], "dp", 1)
    paired = [jnp.concatenate([columns[0, k], swapped[k]], axis=1) for k in range(chips)]
    near = chips // x_count
    low = near.bit_length() - 1
    paired = reorder(paired, ((chip_index // near) ^ x_index) * near, low)
    parts = [0.0] * near
    for k in range(chips):
        moves = []
        for z in range(chips):
            for c in range(2):
                for x in range(x_count):
                    away = (z // near) ^ x
                    there = z ^ k ^ (away * near)
                    moves.append(((2 * z + c) * x_count + x, (2 * there + c) * x_count + z // near))
        got = lax.ppermute(paired[k], ("dp", "expert"), moves).astype(f32)
        parts[k % near] = parts[k % near] + got
    parts = [
        reorder([p[:, c * block : (c + 1) * block] for c in range(2)], core_index)
        for p in reorder(parts, chip_index % near)
    ]
    stream = jnp.concatenate([b for pair in parts for b in pair], axis=1)
    stream = stream + residual.astype(f32).reshape(own, width)

    share = route_weights / jnp.sum(route_weights, axis=2, keepdims=True)
    catalog = jnp.arange(expert_total, dtype=jnp.int32)
    named = expert_ids[..., None] == catalog
    routed = jnp.sum(jnp.where(named, share[..., None], 0.0), axis=2)
    routed_high, routed_low = split_pair(routed.reshape(own, expert_total))
    square_high, square_low = split_pair(jnp.sum(stream * stream, axis=1, keepdims=True))
    extra = -(-(2 * expert_total + 2) // 128) * 128
    rows = jnp.concatenate(
        [
            (stream * norm_gain[None, :]).astype(bf16),
            square_high,
            square_low,
            routed_high,
            routed_low,
            jnp.zeros((own, extra - 2 * expert_total - 2), bf16),
        ],
        axis=1,
    )
    from_chip = [rows] + [exchange(rows, "dp", 2 * k) for k in range(1, chips)]
    result = stream
    for chunk in (range(chips // 2, chips), range(chips // 2)):
        mine = jnp.concatenate([from_chip[k] for k in chunk], axis=0)
        taken = jnp.concatenate([mine, exchange(mine, "dp", 1)], axis=0)
        keep, send = expert_chunk(taken, x_index, dp_index, gate_up, down_proj, expert_total)
        keep = keep + exchange(send, "dp", 1).astype(f32)
        for i, k in enumerate(chunk):
            piece = keep[i * own : (i + 1) * own]
            if k > 0:
                piece = exchange(piece.astype(bf16), "dp", 2 * k).astype(f32)
            result = result + piece
    return result.reshape(steps, reqs, width).astype(bf16)


def body_fast(
    queries,
    fresh_kv,
    kv_pool,
    page_table,
    context_lengths,
    residual,
    out_weight,
    norm_gain,
    expert_ids,
    route_weights,
    gate_up,
    down_proj,
):
    bf16, f32 = jnp.bfloat16, jnp.float32
    dp_count, x_count = lax.axis_size("dp"), lax.axis_size("expert")
    dp_index, x_index = lax.axis_index("dp"), lax.axis_index("expert")
    index = jnp.concatenate([jnp.stack([dp_index, x_index]).astype(jnp.int32), context_lengths])
    chips = dp_count // 2
    local_experts, _, width, hidden = gate_up.shape
    part = hidden // 2
    expert_total = local_experts * dp_count
    steps, reqs = queries.shape[:2]
    own = steps * reqs

    attended, gate_up, down_proj = attend_pool(
        index, queries, fresh_kv, kv_pool, page_table, gate_up, down_proj
    )
    head_cols = attended.shape[1]
    mine = [attended] + [exchange(attended, "dp", 2 * k) for k in range(1, chips)]
    mine = mine + [exchange(piece, "dp", 1) for piece in mine]
    block = out_weight.shape[1]
    keep, send = small_call(
        functools.partial(project_kernel, chips),
        [((chips, own, block), bf16)] * 2,
        *mine,
        out_weight,
        index=index,
        flops=2 * dp_count * own * head_cols * block,
    )
    paired = small_call(
        pair_kernel, [((own, 2 * block), bf16)] * chips, keep, exchange(send, "dp", 1)
    )
    near = chips // x_count
    arrived = []
    for k in range(chips):
        moves = []
        for z in range(chips):
            for c in range(2):
                for x in range(x_count):
                    away = (z // near) ^ x
                    there = z ^ k ^ (away * near)
                    moves.append(((2 * z + c) * x_count + x, (2 * there + c) * x_count + z // near))
        arrived.append(lax.ppermute(paired[k], ("dp", "expert"), moves))

    extra = -(-(2 * expert_total + 2) // 128) * 128
    stream, rows = small_call(
        functools.partial(stream_kernel, chips, expert_total),
        [((own, width), f32), ((own, width + extra), bf16)],
        *arrived,
        residual.reshape(own, width),
        norm_gain.reshape(1, width),
        jnp.swapaxes(expert_ids, 1, 2),
        jnp.swapaxes(route_weights, 1, 2),
        index=index,
    )
    from_chip = [rows]
    for k in range(1, chips):
        from_chip.append(exchange(rows, "dp", 2 * k))
        if k == 1 or k % 2 == 0:
            (from_chip[k],) = small_call(hold_kernel, [(rows.shape, bf16)], from_chip[k])
    result = stream
    for chunk in (range(1, chips, 2), range(0, chips, 2)):
        pieces = [from_chip[k] for k in chunk]
        pieces = pieces + [exchange(piece, "dp", 1) for piece in pieces]
        count = len(pieces) * own
        keep, send, extras = small_call(
            functools.partial(gate_up_kernel, len(pieces)),
            [
                ((2 * local_experts, count, part), f32),
                ((count, 2 * local_experts * part + extra), bf16),
                ((count, extra), bf16),
            ],
            *pieces,
            gate_up,
            index=index,
            flops=4 * count * width * hidden * local_experts,
        )
        got = exchange(send, "expert", 1)
        (act,) = small_call(
            functools.partial(act_kernel, local_experts, expert_total, x_count * width),
            [((count, local_experts * part), bf16)],
            keep,
            got,
            extras,
            index=index,
        )
        got = exchange(act, "expert", 1)
        keep, send = small_call(
            down_kernel,
            [((count // 2, width), f32), ((count // 2, width), bf16)],
            act,
            got,
            down_proj,
            index=index,
            flops=2 * count * width * hidden * local_experts,
        )
        folded = small_call(
            fold_kernel,
            [((own, width), bf16 if k else f32) for k in chunk],
            keep,
            exchange(send, "dp", 1),
        )
        for k, piece in zip(chunk, folded):
            if k > 0:
                piece = exchange(piece, "dp", 2 * k).astype(f32)
            result = result + piece
    return result.reshape(steps, reqs, width).astype(bf16)


def body(*args):
    fast = (
        args[2].shape[2] == 2
        and lax.axis_size("expert") == 2
        and lax.axis_size("dp") >= 4
        and args[10].shape[3] % 256 == 0
        and args[10].shape[2] % 512 == 0
    )
    if not fast:
        return body_plain(*args)
    return body_fast(*args)


def solution(mesh):
    return jax.shard_map(
        body,
        mesh=mesh,
        in_specs=(
            P(None, ("groups", "dp"), "expert", None),
            P(None, ("groups", "dp"), "expert", None),
            P(("groups", "dp"), None, "expert", None),
            P(("groups", "dp"), None),
            P(("groups", "dp")),
            P(None, ("groups", "dp"), "expert"),
            P("expert", "dp"),
            P("expert"),
            P(None, ("groups", "dp"), None),
            P(None, ("groups", "dp"), None),
            P("dp", None, "expert", None),
            P("dp", None, "expert"),
        ),
        out_specs=P(None, ("groups", "dp"), "expert"),
        check_vma=False,
    )
```
